16 devices in a mesh: dp: 2 (over y, z), tp: 8 (over x, core).
Axes of the slice: x: 4, y: 2, z: 1, core: 2. Of those that a mesh axis runs over, the one named last changes fastest.
The devices are a block of a 4x4x8 slice.
Arguments:
- x: bfloat16 [6144, 3584], P(('dp', 'tp')), parts along dimension 0
- gain_a: bfloat16 [3584], replicated
- wq: bfloat16 [3584, 4096], P(None, 'tp')
- wk: bfloat16 [3584, 2048], P(None, 'tp')
- wv: bfloat16 [3584, 2048], P(None, 'tp')
- wo: bfloat16 [4096, 3584], P('tp')
- gain_m: bfloat16 [3584], replicated
- w_gate: bfloat16 [3584, 14336], P(None, 'tp')
- w_up: bfloat16 [3584, 14336], P(None, 'tp')
- w_down: bfloat16 [14336, 3584], P('tp')
Outputs:
- output: bfloat16 [6144, 3584], P(('dp', 'tp')), parts along dimension 0
There are 2 independent parts. The reference program is written for one: setup_inputs(seed, part) draws one part's arguments, and reference() takes and returns one part's arrays. A program takes and returns all parts, laid end to end along the dimension named above; an argument that names none is the same for every part.
All inputs are finite; a program needn't handle non-finite values.
Results may differ from the reference program's by a relative error of at most 0.017.
Values are sent between devices in bfloat16 or wider.
A program may use at most 768 MiB of HBM per device.

```python
import jax
import jax.numpy as jnp
from jax import lax

ROWS = 3072
D = 3584
HEADS = 16
KV_HEADS = 8
HEAD = 256
FF = 14336
THETA = 10000


def setup_inputs(seed: int = 0, part: int = 0) -> dict:
    kx, kn, kq, kk, kv, ko, km, kg, ku, kd = jax.random.split(jax.random.key(seed), 10)

    def weights(key, rows, columns):
        return jax.random.normal(key, (rows, columns), jnp.float32) * rows**-0.5

    drawn = {
        "x": jax.random.normal(jax.random.fold_in(kx, part), (ROWS, D), jnp.float32),
        "gain_a": 1 + 0.1 * jax.random.normal(kn, (D,), jnp.float32),
        "wq": 2 * weights(kq, D, HEADS * HEAD),
        "wk": 2 * weights(kk, D, KV_HEADS * HEAD),
        "wv": 4 * weights(kv, D, KV_HEADS * HEAD),
        "wo": weights(ko, HEADS * HEAD, D),
        "gain_m": 1 + 0.1 * jax.random.normal(km, (D,), jnp.float32),
        "w_gate": weights(kg, D, FF),
        "w_up": weights(ku, D, FF),
        "w_down": 2 * weights(kd, FF, D),
    }
    return {k: v.astype(jnp.bfloat16) for k, v in drawn.items()}


def normed(x, gain):
    wide = x.astype(jnp.float32)
    scale = lax.rsqrt(jnp.mean(wide * wide, -1, keepdims=True) + 1e-6)
    return (wide * scale * gain.astype(jnp.float32)).astype(jnp.bfloat16)


def turned(t, place, theta):
    half = t.shape[-1] // 2
    angle = place.astype(jnp.float32)[:, None] * theta ** (-jnp.arange(half, dtype=jnp.float32) / half)
    cos, sin = jnp.cos(angle)[:, None], jnp.sin(angle)[:, None]
    a, b = t[..., :half].astype(jnp.float32), t[..., half:].astype(jnp.float32)
    return jnp.concatenate([a * cos - b * sin, b * cos + a * sin], -1).astype(jnp.bfloat16)


def matmul(a, w):
    return jnp.dot(a, w, preferred_element_type=jnp.float32).astype(jnp.bfloat16)


def einsum(form, a, b):
    return jnp.einsum(form, a.astype(jnp.float32), b.astype(jnp.float32))


def attention(q, k, v):
    scores = einsum("tgsd,ugd->gstu", q, k) * q.shape[-1] ** -0.5
    token = jnp.arange(q.shape[0])
    scores = jnp.where(token[:, None] >= token, scores, -jnp.inf)
    weights = jax.nn.softmax(scores, -1).astype(jnp.bfloat16)
    return einsum("gstu,ugd->tgsd", weights, v).astype(jnp.bfloat16)


def reference(x, gain_a, wq, wk, wv, wo, gain_m, w_gate, w_up, w_down):
    a, place = normed(x, gain_a), jnp.arange(ROWS)
    q = turned(matmul(a, wq).reshape(ROWS, HEADS, HEAD), place, THETA).reshape(ROWS, KV_HEADS, -1, HEAD)
    k = turned(matmul(a, wk).reshape(ROWS, KV_HEADS, HEAD), place, THETA)
    v = matmul(a, wv).reshape(ROWS, KV_HEADS, HEAD)
    seen = attention(q, k, v).reshape(ROWS, HEADS * HEAD)
    h = (x.astype(jnp.float32) + jnp.dot(seen, wo, preferred_element_type=jnp.float32)).astype(jnp.bfloat16)
    b = normed(h, gain_m)
    gate = jnp.dot(b, w_gate, preferred_element_type=jnp.float32)
    up = jnp.dot(b, w_up, preferred_element_type=jnp.float32)
    hidden = (jax.nn.silu(gate) * up).astype(jnp.bfloat16)
    return (h.astype(jnp.float32) + jnp.dot(hidden, w_down, preferred_element_type=jnp.float32)).astype(jnp.bfloat16)
```

```python
import functools

import jax
import jax.numpy as jnp
from jax import lax
from jax.experimental import pallas as pl
from jax.experimental.pallas import tpu as pltpu
from jax.sharding import PartitionSpec as P


NEG = -1e30
HIDDEN = 2 * NEG
LOG2E = 1.4426950408889634
HEAD = 256
THETA = 10000
BK = 512
WIDE = 256


def _dot(a, b, ca, cb):
    return lax.dot_general(a, b, (((ca,), (cb,)), ((), ())), preferred_element_type=jnp.float32)


def _attend(pos_ref, qa_ref, qb_ref, kv_ref, oa_ref, ob_ref, top_s, mix_s):
    i = pl.program_id(0)
    rows, d = qa_ref.shape[0], HEAD
    heads = qa_ref.shape[1] // d
    cols = 2 * heads * rows
    pa, pb = pos_ref[i], pos_ref[2 + i]
    e = d**-0.5 * LOG2E
    q = jnp.concatenate([r[:, h * d : (h + 1) * d] for r in (qa_ref, qb_ref) for h in range(heads)], axis=0)
    top_s[...] = jnp.full(top_s.shape, NEG, jnp.float32)
    mix_s[...] = jnp.zeros(mix_s.shape, jnp.float32)
    column = lax.broadcasted_iota(jnp.int32, (1, cols), 1)
    place = lax.rem(column, rows) + jnp.where(column < heads * rows, pa, pb)
    low, high = jnp.minimum(pa, pb), jnp.maximum(pa, pb)
    ones = jnp.ones((8, BK), kv_ref.dtype)

    def block(j, masked):
        here = pl.ds(pl.multiple_of(j * BK, BK), BK)
        keys = kv_ref[here, :d]
        values = jnp.concatenate([kv_ref[here, d:].T, ones], axis=0)
        strips = range(0, cols, WIDE)
        scores = [_dot(keys, q[at : at + WIDE, :], 1, 1) for at in strips]
        weights, keeps = [], []
        for at, s in zip(strips, scores):
            if masked:
                key = lax.broadcasted_iota(jnp.int32, s.shape, 0) + j * BK
                s = jnp.where(key <= place[:, at : at + WIDE], s, HIDDEN)
            old = top_s[:, at : at + WIDE]
            top = jnp.maximum(old, s.max(axis=0, keepdims=True))
            top_s[:, at : at + WIDE] = top
            weights.append(jnp.exp2((s - top) * e).astype(kv_ref.dtype))
            keeps.append(jnp.exp2((old - top) * e))
        for at, p, keep in zip(strips, weights, keeps):
            mix_s[:, at : at + WIDE] = mix_s[:, at : at + WIDE] * keep + _dot(values, p, 1, 0)

    whole = lax.div(low + 1, BK)
    last = lax.div(high + rows + BK - 1, BK)
    lax.fori_loop(0, whole, lambda j, _: block(j, False), None)
    lax.fori_loop(whole, last, lambda j, _: block(j, True), None)
    out = (mix_s[:d, :] * (1 / mix_s[d : d + 1, :])).T.astype(oa_ref.dtype)
    for n, ref in enumerate((oa_ref, ob_ref)):
        for h in range(heads):
            at = (n * heads + h) * rows
            ref[:, h * d : (h + 1) * d] = out[at : at + rows, :]


def attend(q, kv, pos):
    rows, width = q.shape[0] // 4, q.shape[1]
    tokens = kv.shape[0]
    cols = 2 * (width // HEAD) * rows
    out = jax.ShapeDtypeStruct((2 * rows, width), q.dtype)
    return pl.pallas_call(
        _attend,
        grid_spec=pltpu.PrefetchScalarGridSpec(
            num_scalar_prefetch=1,
            grid=(2,),
            in_specs=[
                pl.BlockSpec((rows, width), lambda i, _: (i, 0)),
                pl.BlockSpec((rows, width), lambda i, _: (2 + i, 0)),
                pl.BlockSpec((tokens, 2 * HEAD), lambda i, _: (0, 0)),
            ],
            out_specs=[pl.BlockSpec((rows, width), lambda i, _: (i, 0))] * 2,
            scratch_shapes=[pltpu.VMEM((1, cols), jnp.float32), pltpu.VMEM((HEAD + 8, cols), jnp.float32)],
        ),
        out_shape=[out, out],
        compiler_params=pltpu.CompilerParams(dimension_semantics=("arbitrary",), vmem_limit_bytes=40 * 2**20),
        cost_estimate=pl.CostEstimate(flops=2 * 4 * rows * width * tokens, transcendentals=2 * rows * width // HEAD * tokens,
                                      bytes_accessed=2 * (2 * q.size + kv.size)),
    )(pos, q, q, kv)


def normed(x, gain):
    wide = x.astype(jnp.float32)
    scale = lax.rsqrt(jnp.mean(wide * wide, -1, keepdims=True) + 1e-6)
    return (wide * scale * gain.astype(jnp.float32)).astype(jnp.bfloat16)


def turned(t, cos, sin):
    half = HEAD // 2
    parts = []
    for at in range(0, t.shape[1], HEAD):
        a, b = t[:, at : at + half].astype(jnp.float32), t[:, at + half : at + HEAD].astype(jnp.float32)
        parts += [a * cos - b * sin, b * cos + a * sin]
    return jnp.concatenate(parts, -1).astype(jnp.bfloat16)


def dot(a, w):
    return jnp.dot(a, w, preferred_element_type=jnp.float32)


def low(t):
    return t.astype(jnp.bfloat16)


def wide(t):
    return t.astype(jnp.float32)


def solution(mesh):
    n = mesh.shape["tp"]

    def sender(to):
        pairs = [(i, to(i)) for i in range(n)]
        return lambda t: lax.ppermute(t, "tp", pairs)

    to_right, to_left = sender(lambda i: (i + 2) % n), sender(lambda i: (i - 2) % n)
    swap = sender(lambda i: i ^ 1)

    def gathered(top, bottom):
        left_top, right_bottom = to_right(top), to_left(bottom)
        left_bottom, right_top = to_right(bottom), to_left(top)
        far_top, far_bottom = to_right(left_top), to_left(right_bottom)
        sets = []
        for a, b in ((top, bottom), (left_top, right_bottom), (right_top, left_bottom), (far_top, far_bottom)):
            sets.append(jnp.concatenate([a, b, swap(a), swap(b)], 0))
        return sets

    def summed(terms, w):
        own, first, second, far = terms

        def chip(term, extra=None):
            mine, other = term
            total = dot(mine, w) + wide(swap(low(dot(other, w))))
            return total if extra is None else total + extra

        half = own[0].shape[0] // 2
        t = low(chip(first))
        top_direct, bottom_direct = to_left(t[:half]), to_right(t[half:])
        t = low(chip(far))
        top_far, bottom_far = to_right(t[:half]), to_left(t[half:])
        t = low(chip(second, wide(jnp.concatenate([top_far, bottom_far], 0))))
        top_near, bottom_near = to_right(t[:half]), to_left(t[half:])
        return chip(own, wide(jnp.concatenate([top_direct, bottom_direct], 0)) + wide(jnp.concatenate([top_near, bottom_near], 0)))

    def step(x, gain_a, wq, wk, wv, wo, gain_m, w_gate, w_up, w_down):
        me = lax.axis_index("tp")
        rows = x.shape[0]
        half = rows // 2
        chip, core = me // 2, me % 2

        def places(shift_a, at_a, shift_b, at_b):
            def place(shift, other, at):
                return ((chip * 2 + 2 * shift) % n + (core ^ other)) * rows + at * half
            return jnp.stack([place(shift_a, 0, at_a), place(shift_b, 0, at_b), place(shift_a, 1, at_a), place(shift_b, 1, at_b)])

        places_of = [places(0, 0, 0, 1), places(-1, 0, 1, 1), places(1, 0, -1, 1), places(2, 0, 2, 1)]

        a = normed(x, gain_a)
        sets = gathered(a[:half], a[half:])
        w = jnp.concatenate([wq, wk, wv], 1)
        queries = wq.shape[1]
        kv = jnp.zeros((rows * n, 2 * HEAD), jnp.bfloat16)
        qs = []
        frequency = THETA ** (-jnp.arange(HEAD // 2, dtype=jnp.float32) / (HEAD // 2))
        for s, p in zip(sets, places_of):
            t = low(dot(s, w))
            place = (p[:, None] + jnp.arange(half)).reshape(-1)
            angle = place.astype(jnp.float32)[:, None] * frequency
            r = turned(t[:, : queries + HEAD], jnp.cos(angle), jnp.sin(angle))
            qs.append(r[:, :queries])
            both = jnp.concatenate([r[:, queries:], t[:, queries + HEAD :]], 1)
            for i in range(4):
                kv = lax.dynamic_update_slice(kv, both[i * half : (i + 1) * half], (p[i], 0))
        own, first, second, far = range(4)
        seen = {}
        for i in (first, far, second, own):
            seen[i] = attend(qs[i], kv, places_of[i])
        h = low(wide(x) + summed([seen[i] for i in range(4)], wo))

        b = normed(h, gain_m)
        sets = gathered(b[:half], b[half:])
        hidden = {}
        for i in (own, first, second, far):
            t = low(jax.nn.silu(dot(sets[i], w_gate)) * dot(sets[i], w_up))
            hidden[i] = t[:rows], t[rows:]
        return low(wide(h) + summed([hidden[i] for i in range(4)], w_down))

    tokens, columns, rows_of = P(("dp", "tp"), None), P(None, "tp"), P("tp", None)
    return jax.shard_map(
        step,
        mesh=mesh,
        in_specs=(tokens, P(None), columns, columns, columns, rows_of, P(None), columns, columns, rows_of),
        out_specs=tokens,
        check_vma=False,
    )
```

```python
import functools

import jax
import jax.numpy as jnp
from jax import lax
from jax.experimental import pallas as pl
from jax.experimental.pallas import tpu as pltpu
from jax.sharding import PartitionSpec as P


NEG = -1e30
HIDDEN = 2 * NEG
LOG2E = 1.4426950408889634
HEAD = 256
THETA = 10000
BK = 512
WIDE = 256


def _dot(a, b, ca, cb):
    return lax.dot_general(a, b, (((ca,), (cb,)), ((), ())), preferred_element_type=jnp.float32)


def _attend(pos_ref, qa_ref, qb_ref, kv_ref, oa_ref, ob_ref, top_s, mix_s):
    i = pl.program_id(0)
    rows, d = qa_ref.shape[0], HEAD
    heads = qa_ref.shape[1] // d
    cols = 2 * heads * rows
    pa, pb = pos_ref[i], pos_ref[2 + i]
    e = d**-0.5 * LOG2E
    q = jnp.concatenate([r[:, h * d : (h + 1) * d] for r in (qa_ref, qb_ref) for h in range(heads)], axis=0)
    top_s[...] = jnp.full(top_s.shape, NEG, jnp.float32)
    mix_s[...] = jnp.zeros(mix_s.shape, jnp.float32)
    column = lax.broadcasted_iota(jnp.int32, (1, cols), 1)
    place = lax.rem(column, rows) + jnp.where(column < heads * rows, pa, pb)
    low, high = jnp.minimum(pa, pb), jnp.maximum(pa, pb)
    ones = jnp.ones((8, BK), kv_ref.dtype)

    def block(j, masked):
        here = pl.ds(pl.multiple_of(j * BK, BK), BK)
        keys = kv_ref[here, :d]
        values = jnp.concatenate([kv_ref[here, d:].T, ones], axis=0)
        strips = range(0, cols, WIDE)
        scores = [_dot(keys, q[at : at + WIDE, :], 1, 1) for at in strips]
        weights, keeps = [], []
        for at, s in zip(strips, scores):
            if masked:
                key = lax.broadcasted_iota(jnp.int32, s.shape, 0) + j * BK
                s = jnp.where(key <= place[:, at : at + WIDE], s, HIDDEN)
            old = top_s[:, at : at + WIDE]
            top = jnp.maximum(old, s.max(axis=0, keepdims=True))
            top_s[:, at : at + WIDE] = top
            weights.append(jnp.exp2((s - top) * e).astype(kv_ref.dtype))
            keeps.append(jnp.exp2((old - top) * e))
        for at, p, keep in zip(strips, weights, keeps):
            mix_s[:, at : at + WIDE] = mix_s[:, at : at + WIDE] * keep + _dot(values, p, 1, 0)

    whole = lax.div(low + 1, BK)
    last = lax.div(high + rows + BK - 1, BK)
    lax.fori_loop(0, whole, lambda j, _: block(j, False), None)
    lax.fori_loop(whole, last, lambda j, _: block(j, True), None)
    out = (mix_s[:d, :] * (1 / mix_s[d : d + 1, :])).T.astype(oa_ref.dtype)
    for n, ref in enumerate((oa_ref, ob_ref)):
        for h in range(heads):
            at = (n * heads + h) * rows
            ref[:, h * d : (h + 1) * d] = out[at : at + rows, :]


def attend(q, kv, pos):
    rows, width = q.shape[0] // 4, q.shape[1]
    tokens = kv.shape[0]
    cols = 2 * (width // HEAD) * rows
    out = jax.ShapeDtypeStruct((2 * rows, width), q.dtype)
    return pl.pallas_call(
        _attend,
        grid_spec=pltpu.PrefetchScalarGridSpec(
            num_scalar_prefetch=1,
            grid=(2,),
            in_specs=[
                pl.BlockSpec((rows, width), lambda i, _: (i, 0)),
                pl.BlockSpec((rows, width), lambda i, _: (2 + i, 0)),
                pl.BlockSpec((tokens, 2 * HEAD), lambda i, _: (0, 0)),
            ],
            out_specs=[pl.BlockSpec((rows, width), lambda i, _: (i, 0))] * 2,
            scratch_shapes=[pltpu.VMEM((1, cols), jnp.float32), pltpu.VMEM((HEAD + 8, cols), jnp.float32)],
        ),
        out_shape=[out, out],
        compiler_params=pltpu.CompilerParams(dimension_semantics=("arbitrary",), vmem_limit_bytes=40 * 2**20),
        cost_estimate=pl.CostEstimate(flops=2 * 4 * rows * width * tokens, transcendentals=2 * rows * width // HEAD * tokens,
                                      bytes_accessed=2 * (2 * q.size + kv.size)),
    )(pos, q, q, kv)


MESH = pl.DeviceIdType.MESH
FULL = 67_043_328
COLS = 512
HIDE = 256
OWN, FIRST, SECOND, FAR = range(4)


def _around(n):
    me = lax.axis_index("tp")
    return lax.rem(me + 2, n), lax.rem(me + n - 2, n), me + 1 - 2 * lax.rem(me, 2)


def _enter(*others):
    barrier = pltpu.get_barrier_semaphore()
    for other in others:
        pl.semaphore_signal(barrier, inc=1, device_id={"tp": other}, device_id_type=MESH)
    pl.semaphore_wait(barrier, len(others))


class Gather:
    def __init__(self, g, send, recv, around):
        self.g, self.sems, self.around = g, (send, recv), around

    def copy(self, source, slot, to):
        right, left, twin = self.around
        return pltpu.make_async_remote_copy(
            src_ref=self.g.at[source], dst_ref=self.g.at[slot], send_sem=self.sems[0].at[slot], recv_sem=self.sems[1].at[slot],
            device_id={"tp": {"right": right, "left": left, "twin": twin}[to]}, device_id_type=MESH)

    PATH = {4: (0, "right"), 5: (1, "left"), 9: (1, "right"), 8: (0, "left"), 12: (4, "right"), 13: (5, "left"),
            2: (0, "twin"), 3: (1, "twin"), 6: (4, "twin"), 7: (5, "twin"), 10: (8, "twin"), 11: (9, "twin"), 14: (12, "twin"), 15: (13, "twin")}

    def start(self, *slots):
        for slot in slots:
            source, to = self.PATH[slot]
            self.copy(source, slot, to).start()

    def arrived(self, *slots):
        for slot in slots:
            source, to = self.PATH[slot]
            self.copy(source, slot, to).wait_recv()

    def sent(self, *slots):
        for slot in slots:
            source, to = self.PATH[slot]
            self.copy(source, slot, to).wait_send()


class Scatter:
    def __init__(self, g, swapped, direct, passed, near, sems, around):
        self.g, self.swapped, self.direct, self.passed, self.near, self.around = g, swapped, direct, passed, near, around
        self.swap_send, self.swap_recv, self.send, self.recv = sems
        self.steps = g.shape[2] // COLS

    def cols(self, n):
        return pl.ds(pl.multiple_of(n * COLS, COLS), COLS)

    def swap(self, s, stage, n):
        at = pl.ds(0, self.g.shape[2]) if n is None else self.cols(n)
        return pltpu.make_async_remote_copy(
            src_ref=self.g.at[pl.ds(stage, 2), :, at], dst_ref=self.swapped.at[s, :, :, at], send_sem=self.swap_send.at[s],
            recv_sem=self.swap_recv.at[s * self.steps + (0 if n is None else n)], device_id={"tp": self.around[2]}, device_id_type=MESH)

    def hop(self, s, stage, piece, n):
        right, left, _ = self.around
        to = left if (s == FIRST) == (piece == 0) else right
        buffer = {FIRST: self.direct, FAR: self.passed, SECOND: self.near}[s]
        at = pl.ds(0, self.g.shape[2]) if n is None else self.cols(n)
        k = {FIRST: 0, FAR: 1, SECOND: 2}[s] * 2 + piece
        return pltpu.make_async_remote_copy(
            src_ref=self.g.at[stage + piece, :, at], dst_ref=buffer.at[piece, :, at], send_sem=self.send.at[k],
            recv_sem=self.recv.at[k * self.steps + (0 if n is None else n)], device_id={"tp": to}, device_id_type=MESH)

    def others(self, s, stage, term):
        def body(n, _):
            t = term(n)
            half = t.shape[0] // 2
            self.g[stage, :, self.cols(n)] = t[:half].astype(self.g.dtype)
            self.g[stage + 1, :, self.cols(n)] = t[half:].astype(self.g.dtype)

            @pl.when(n > 0)
            def _():
                self.swap(s, stage, n - 1).start()

        lax.fori_loop(0, self.steps, body, None)
        self.swap(s, stage, self.steps - 1).start()

    def mine(self, s, stage, term):
        def body(n, _):
            t = term(n)
            half = t.shape[0] // 2
            self.swap(s, stage, n).wait_recv()
            for piece in range(2):
                total = t[piece * half : (piece + 1) * half] + self.swapped[s, piece, :, self.cols(n)].astype(jnp.float32)
                if s == SECOND:
                    self.hop(FAR, stage, piece, n).wait_recv()
                    total += self.passed[piece, :, self.cols(n)].astype(jnp.float32)
                self.g[stage + piece, :, self.cols(n)] = total.astype(self.g.dtype)

            @pl.when(n > 0)
            def _():
                for piece in range(2):
                    self.hop(s, stage, piece, n - 1).start()

        lax.fori_loop(0, self.steps, body, None)
        for piece in range(2):
            self.hop(s, stage, piece, self.steps - 1).start()

    def finish(self, stage, term, out, out_sem):
        def whole(n, piece):
            return pltpu.make_async_copy(self.g.at[stage + piece, :, self.cols(n)], out.at[piece, :, self.cols(n)], out_sem.at[n * 2 + piece])

        def early(n, _):
            for piece in range(2):
                self.hop(FIRST, stage, piece, n).wait_recv()

        lax.fori_loop(0, self.steps, early, None)

        def body(n, _):
            t = term(n)
            half = t.shape[0] // 2
            self.swap(OWN, stage, n).wait_recv()
            for piece in range(2):
                total = t[piece * half : (piece + 1) * half] + self.swapped[OWN, piece, :, self.cols(n)].astype(jnp.float32)
                total += self.direct[piece, :, self.cols(n)].astype(jnp.float32)
                self.hop(SECOND, stage, piece, n).wait_recv()
                total += self.near[piece, :, self.cols(n)].astype(jnp.float32)
                total += self.g[stage + piece, :, self.cols(n)].astype(jnp.float32)
                self.g[stage + piece, :, self.cols(n)] = total.astype(self.g.dtype)

            @pl.when(n > 0)
            def _():
                for piece in range(2):
                    whole(n - 1, piece).start()

        lax.fori_loop(0, self.steps, body, None)
        for piece in range(2):
            whole(self.steps - 1, piece).start()

        def end(n, _):
            for piece in range(2):
                whole(n, piece).wait()

        lax.fori_loop(0, self.steps, end, None)


def _norm(g, gain_ref):
    step = 16
    per = g.shape[1] // step
    gain = gain_ref[...].astype(jnp.float32)

    def body(i, _):
        at = pl.ds(pl.multiple_of(lax.rem(i, per) * step, step), step)
        t = g[lax.div(i, per), at, :].astype(jnp.float32)
        scale = lax.rsqrt(jnp.mean(t * t, -1, keepdims=True) + 1e-6)
        g[lax.div(i, per), at, :] = (t * scale * gain).astype(g.dtype)

    lax.fori_loop(0, 2 * per, body, None)


def _mlp(n, h_ref, gain_ref, gate_ref, up_ref, down_ref, y_ref, g, swapped, direct, passed, near, hid, wgu, wd,
         g_send, g_recv, swap_send, swap_recv, hop_send, hop_recv, w_sem, io_sem, out_sem):
    around = _around(n)
    gather = Gather(g, g_send, g_recv, around)
    scatter = Scatter(g, swapped, direct, passed, near, (swap_send, swap_recv, hop_send, hop_recv), around)
    rows = 2 * g.shape[1]
    depth = g.shape[2]
    units = gate_ref.shape[1]
    tiles, steps = units // HIDE, scatter.steps

    def fetch(i, slot):
        at = pl.ds(pl.multiple_of(i * HIDE, HIDE), HIDE)
        return [pltpu.make_async_copy(ref.at[:, at], wgu.at[slot, k], w_sem.at[slot * 2 + k]) for k, ref in enumerate((gate_ref, up_ref))]

    def fetch_down(i, slot):
        return pltpu.make_async_copy(down_ref.at[:, scatter.cols(i)], wd.at[slot], w_sem.at[4 + slot])

    def hidden(s, place, more):
        def body(i, _):
            slot = lax.rem(i, 2)

            @pl.when(i + 1 < tiles)
            def _():
                for c in fetch(i + 1, 1 - slot):
                    c.start()

            for c in fetch(i, slot):
                c.wait()
            at = pl.ds(pl.multiple_of(i * HIDE, HIDE), HIDE)
            for part in range(2):
                t = g[4 * s + 2 * part : 4 * s + 2 * part + 2].reshape(rows, depth)
                gate = jnp.dot(t, wgu[slot, 0], preferred_element_type=jnp.float32)
                up = jnp.dot(t, wgu[slot, 1], preferred_element_type=jnp.float32)
                hid[place, part * rows : (part + 1) * rows, at] = (gate / (1 + jnp.exp(-gate)) * up).astype(hid.dtype)

        lax.fori_loop(0, tiles, body, None)
        if more:
            for c in fetch(0, 0):
                c.start()

    def down(place, part, more=True):
        def term(i):
            slot = lax.rem(i, 2)

            @pl.when(i + 1 < steps)
            def _():
                fetch_down(i + 1, 1 - slot).start()

            fetch_down(i, slot).wait()
            t = jnp.dot(hid[place, part * rows : (part + 1) * rows, :], wd[slot], preferred_element_type=jnp.float32)
            return t

        return term

    def again():
        fetch_down(0, 0).start()

    load = pltpu.make_async_copy(h_ref, g.at[pl.ds(0, 2)], io_sem.at[0])
    load.start()
    for c in fetch(0, 0):
        c.start()
    again()
    _enter(*around)
    load.wait()
    _norm(g, gain_ref)
    gather.start(4, 5, 2, 3, 9, 8)
    gather.arrived(2, 3)
    hidden(OWN, 1, True)
    gather.arrived(4, 5)
    gather.start(12, 13, 6, 7)
    gather.arrived(6, 7)
    hidden(FIRST, 0, True)
    gather.sent(4, 5, 2, 3, 9, 8)
    scatter.others(FIRST, 2, down(0, 1))
    again()
    gather.arrived(8, 9)
    gather.start(10, 11)
    scatter.mine(FIRST, 0, down(0, 0))
    again()
    gather.arrived(10, 11)
    hidden(SECOND, 2, True)
    gather.arrived(12, 13)
    gather.start(14, 15)
    gather.arrived(14, 15)
    hidden(FAR, 0, False)
    gather.sent(12, 13, 6, 7, 10, 11, 14, 15)
    load = pltpu.make_async_copy(h_ref, g.at[pl.ds(12, 2)], io_sem.at[0])
    load.start()
    scatter.others(FAR, 6, down(0, 1))
    again()
    scatter.mine(FAR, 4, down(0, 0))
    again()
    scatter.others(SECOND, 10, down(2, 1))
    again()
    scatter.mine(SECOND, 8, down(2, 0))
    again()
    scatter.others(OWN, 14, down(1, 1))
    again()
    load.wait()
    scatter.finish(12, down(1, 0), y_ref, out_sem)
    for s, stage in ((FIRST, 2), (FAR, 6), (SECOND, 10), (OWN, 14)):
        scatter.swap(s, stage, None).wait_send()
    for s, stage in ((FIRST, 0), (FAR, 4), (SECOND, 8)):
        for piece in range(2):
            scatter.hop(s, stage, piece, None).wait_send()


def _buffers(half, depth):
    piece = lambda k: pltpu.VMEM((k, half, depth), jnp.bfloat16)
    steps = depth // COLS
    buffers = [piece(16), pltpu.VMEM((4, 2, half, depth), jnp.bfloat16), piece(2), piece(2), piece(2)]
    sems = [pltpu.SemaphoreType.DMA((k,)) for k in (16, 16, 4, 4 * steps, 6, 6 * steps)]
    return buffers, sems


def mlp(n, h, gain, gate, up, down):
    rows, depth = h.shape
    half = rows // 2
    units = gate.shape[1]
    buffers, sems = _buffers(half, depth)
    any_space = pl.BlockSpec(memory_space=pl.ANY)
    y = pl.pallas_call(
        functools.partial(_mlp, n),
        out_shape=jax.ShapeDtypeStruct((2, half, depth), h.dtype),
        in_specs=[any_space, pl.BlockSpec(memory_space=pltpu.VMEM), any_space, any_space, any_space],
        out_specs=any_space,
        scratch_shapes=[*buffers, pltpu.VMEM((3, 2 * rows, units), h.dtype), pltpu.VMEM((2, 2, depth, HIDE), h.dtype),
                        pltpu.VMEM((2, units, COLS), h.dtype), *sems, pltpu.SemaphoreType.DMA((6,)), pltpu.SemaphoreType.DMA((1,)),
                        pltpu.SemaphoreType.DMA((2 * depth // COLS,))],
        compiler_params=pltpu.CompilerParams(collective_id=1, has_side_effects=True, vmem_limit_bytes=FULL),
        cost_estimate=pl.CostEstimate(flops=6 * rows * n * depth * units, transcendentals=rows * n * units,
                                      bytes_accessed=12 * depth * units),
    )(h.reshape(2, half, depth), gain.reshape(1, depth), gate, up, down)
    return y.reshape(rows, depth)


def normed(x, gain):
    wide = x.astype(jnp.float32)
    scale = lax.rsqrt(jnp.mean(wide * wide, -1, keepdims=True) + 1e-6)
    return (wide * scale * gain.astype(jnp.float32)).astype(jnp.bfloat16)


def turned(t, cos, sin):
    half = HEAD // 2
    parts = []
    for at in range(0, t.shape[1], HEAD):
        a, b = t[:, at : at + half].astype(jnp.float32), t[:, at + half : at + HEAD].astype(jnp.float32)
        parts += [a * cos - b * sin, b * cos + a * sin]
    return jnp.concatenate(parts, -1).astype(jnp.bfloat16)


def dot(a, w):
    return jnp.dot(a, w, preferred_element_type=jnp.float32)


def low(t):
    return t.astype(jnp.bfloat16)


def wide(t):
    return t.astype(jnp.float32)


def solution(mesh):
    n = mesh.shape["tp"]

    def sender(to):
        pairs = [(i, to(i)) for i in range(n)]
        return lambda t: lax.ppermute(t, "tp", pairs)

    to_right, to_left = sender(lambda i: (i + 2) % n), sender(lambda i: (i - 2) % n)
    swap = sender(lambda i: i ^ 1)

    def gathered(top, bottom):
        left_top, right_bottom = to_right(top), to_left(bottom)
        left_bottom, right_top = to_right(bottom), to_left(top)
        far_top, far_bottom = to_right(left_top), to_left(right_bottom)
        sets = []
        for a, b in ((top, bottom), (left_top, right_bottom), (right_top, left_bottom), (far_top, far_bottom)):
            sets.append(jnp.concatenate([a, b, swap(a), swap(b)], 0))
        return sets

    def summed(terms, w):
        own, first, second, far = terms

        def chip(term, extra=None):
            mine, other = term
            total = dot(mine, w) + wide(swap(low(dot(other, w))))
            return total if extra is None else total + extra

        half = own[0].shape[0] // 2
        t = low(chip(first))
        top_direct, bottom_direct = to_left(t[:half]), to_right(t[half:])
        t = low(chip(far))
        top_far, bottom_far = to_right(t[:half]), to_left(t[half:])
        t = low(chip(second, wide(jnp.concatenate([top_far, bottom_far], 0))))
        top_near, bottom_near = to_right(t[:half]), to_left(t[half:])
        return chip(own, wide(jnp.concatenate([top_direct, bottom_direct], 0)) + wide(jnp.concatenate([top_near, bottom_near], 0)))

    def step(x, gain_a, wq, wk, wv, wo, gain_m, w_gate, w_up, w_down):
        me = lax.axis_index("tp")
        rows = x.shape[0]
        half = rows // 2
        chip, core = me // 2, me % 2

        def places(shift_a, at_a, shift_b, at_b):
            def place(shift, other, at):
                return ((chip * 2 + 2 * shift) % n + (core ^ other)) * rows + at * half
            return jnp.stack([place(shift_a, 0, at_a), place(shift_b, 0, at_b), place(shift_a, 1, at_a), place(shift_b, 1, at_b)])

        places_of = [places(0, 0, 0, 1), places(-1, 0, 1, 1), places(1, 0, -1, 1), places(2, 0, 2, 1)]

        a = normed(x, gain_a)
        sets = gathered(a[:half], a[half:])
        w = jnp.concatenate([wq, wk, wv], 1)
        queries = wq.shape[1]
        kv = jnp.zeros((rows * n, 2 * HEAD), jnp.bfloat16)
        qs = []
        frequency = THETA ** (-jnp.arange(HEAD // 2, dtype=jnp.float32) / (HEAD // 2))
        for s, p in zip(sets, places_of):
            t = low(dot(s, w))
            place = (p[:, None] + jnp.arange(half)).reshape(-1)
            angle = place.astype(jnp.float32)[:, None] * frequency
            r = turned(t[:, : queries + HEAD], jnp.cos(angle), jnp.sin(angle))
            qs.append(r[:, :queries])
            both = jnp.concatenate([r[:, queries:], t[:, queries + HEAD :]], 1)
            for i in range(4):
                kv = lax.dynamic_update_slice(kv, both[i * half : (i + 1) * half], (p[i], 0))
        own, first, second, far = range(4)
        seen = {}
        for i in (first, far, second, own):
            seen[i] = attend(qs[i], kv, places_of[i])
        h = low(wide(x) + summed([seen[i] for i in range(4)], wo))

        return mlp(n, h, gain_m, w_gate, w_up, w_down)

    tokens, columns, rows_of = P(("dp", "tp"), None), P(None, "tp"), P("tp", None)
    return jax.shard_map(
        step,
        mesh=mesh,
        in_specs=(tokens, P(None), columns, columns, columns, rows_of, P(None), columns, columns, rows_of),
        out_specs=tokens,
        check_vma=False,
    )
```

```python
import functools

import jax
import jax.numpy as jnp
from jax import lax
from jax.experimental import pallas as pl
from jax.experimental.pallas import tpu as pltpu
from jax.sharding import PartitionSpec as P

NEG = -1e30
HIDDEN = 2 * NEG
LOG2E = 1.4426950408889634
HEAD = 256
THETA = 10000
BK = 256
WIDE = 256


def _dot(a, b, ca, cb):
    return lax.dot_general(a, b, (((ca,), (cb,)), ((), ())), preferred_element_type=jnp.float32)


MESH = pl.DeviceIdType.MESH
FULL = 67_043_328
COLS = 512
HIDE = 256
OWN, FIRST, SECOND, FAR = range(4)


def _around(n):
    me = lax.axis_index("tp")
    return lax.rem(me + 2, n), lax.rem(me + n - 2, n), me + 1 - 2 * lax.rem(me, 2)


def _enter(*others):
    barrier = pltpu.get_barrier_semaphore()
    for other in others:
        pl.semaphore_signal(barrier, inc=1, device_id={"tp": other}, device_id_type=MESH)
    pl.semaphore_wait(barrier, len(others))


class Gather:
    def __init__(self, g, send, recv, around):
        self.g, self.sems, self.around = g, (send, recv), around

    def copy(self, source, slot, to):
        right, left, twin = self.around
        return pltpu.make_async_remote_copy(
            src_ref=self.g.at[source], dst_ref=self.g.at[slot], send_sem=self.sems[0].at[slot], recv_sem=self.sems[1].at[slot],
            device_id={"tp": {"right": right, "left": left, "twin": twin}[to]}, device_id_type=MESH)

    PATH = {4: (0, "right"), 5: (1, "left"), 9: (1, "right"), 8: (0, "left"), 12: (4, "right"), 13: (5, "left"),
            2: (0, "twin"), 3: (1, "twin"), 6: (4, "twin"), 7: (5, "twin"), 10: (8, "twin"), 11: (9, "twin"), 14: (12, "twin"), 15: (13, "twin")}

    def start(self, *slots):
        for slot in slots:
            source, to = self.PATH[slot]
            self.copy(source, slot, to).start()

    def arrived(self, *slots):
        for slot in slots:
            source, to = self.PATH[slot]
            self.copy(source, slot, to).wait_recv()

    def sent(self, *slots):
        for slot in slots:
            source, to = self.PATH[slot]
            self.copy(source, slot, to).wait_send()


class Scatter:
    def __init__(self, g, swapped, direct, passed, near, sems, around):
        self.g, self.swapped, self.direct, self.passed, self.near, self.around = g, swapped, direct, passed, near, around
        self.swap_send, self.swap_recv, self.send, self.recv = sems
        self.steps = g.shape[2] // COLS

    def cols(self, n):
        return pl.ds(pl.multiple_of(n * COLS, COLS), COLS)

    def swap(self, s, stage, n):
        at = pl.ds(0, self.g.shape[2]) if n is None else self.cols(n)
        return pltpu.make_async_remote_copy(
            src_ref=self.g.at[pl.ds(stage, 2), :, at], dst_ref=self.swapped.at[s, :, :, at], send_sem=self.swap_send.at[s],
            recv_sem=self.swap_recv.at[s * self.steps + (0 if n is None else n)], device_id={"tp": self.around[2]}, device_id_type=MESH)

    def hop(self, s, stage, piece, n):
        right, left, _ = self.around
        to = left if (s == FIRST) == (piece == 0) else right
        buffer = {FIRST: self.direct, FAR: self.passed, SECOND: self.near}[s]
        at = pl.ds(0, self.g.shape[2]) if n is None else self.cols(n)
        k = {FIRST: 0, FAR: 1, SECOND: 2}[s] * 2 + piece
        return pltpu.make_async_remote_copy(
            src_ref=self.g.at[stage + piece, :, at], dst_ref=buffer.at[piece, :, at], send_sem=self.send.at[k],
            recv_sem=self.recv.at[k * self.steps + (0 if n is None else n)], device_id={"tp": to}, device_id_type=MESH)

    def others(self, s, stage, term):
        def body(n, _):
            t = term(n)
            half = t.shape[0] // 2
            self.g[stage, :, self.cols(n)] = t[:half].astype(self.g.dtype)
            self.g[stage + 1, :, self.cols(n)] = t[half:].astype(self.g.dtype)

            @pl.when(n > 0)
            def _():
                self.swap(s, stage, n - 1).start()

        lax.fori_loop(0, self.steps, body, None)
        self.swap(s, stage, self.steps - 1).start()

    def mine(self, s, stage, term):
        def body(n, _):
            t = term(n)
            half = t.shape[0] // 2
            self.swap(s, stage, n).wait_recv()
            for piece in range(2):
                total = t[piece * half : (piece + 1) * half] + self.swapped[s, piece, :, self.cols(n)].astype(jnp.float32)
                if s == SECOND:
                    self.hop(FAR, stage, piece, n).wait_recv()
                    total += self.passed[piece, :, self.cols(n)].astype(jnp.float32)
                self.g[stage + piece, :, self.cols(n)] = total.astype(self.g.dtype)

            @pl.when(n > 0)
            def _():
                for piece in range(2):
                    self.hop(s, stage, piece, n - 1).start()

        lax.fori_loop(0, self.steps, body, None)
        for piece in range(2):
            self.hop(s, stage, piece, self.steps - 1).start()

    def finish(self, stage, term, out, out_sem):
        def whole(n, piece):
            return pltpu.make_async_copy(self.g.at[stage + piece, :, self.cols(n)], out.at[piece, :, self.cols(n)], out_sem.at[n * 2 + piece])

        def early(n, _):
            for piece in range(2):
                self.hop(FIRST, stage, piece, n).wait_recv()

        lax.fori_loop(0, self.steps, early, None)

        def body(n, _):
            t = term(n)
            half = t.shape[0] // 2
            self.swap(OWN, stage, n).wait_recv()
            for piece in range(2):
                total = t[piece * half : (piece + 1) * half] + self.swapped[OWN, piece, :, self.cols(n)].astype(jnp.float32)
                total += self.direct[piece, :, self.cols(n)].astype(jnp.float32)
                self.hop(SECOND, stage, piece, n).wait_recv()
                total += self.near[piece, :, self.cols(n)].astype(jnp.float32)
                total += self.g[stage + piece, :, self.cols(n)].astype(jnp.float32)
                self.g[stage + piece, :, self.cols(n)] = total.astype(self.g.dtype)

            @pl.when(n > 0)
            def _():
                for piece in range(2):
                    whole(n - 1, piece).start()

        lax.fori_loop(0, self.steps, body, None)
        for piece in range(2):
            whole(self.steps - 1, piece).start()

        def end(n, _):
            for piece in range(2):
                whole(n, piece).wait()

        lax.fori_loop(0, self.steps, end, None)

    def sent(self):
        for s, stage in ((FIRST, 2), (FAR, 6), (SECOND, 10), (OWN, 14)):
            self.swap(s, stage, None).wait_send()
        for s, stage in ((FIRST, 0), (FAR, 4), (SECOND, 8)):
            for piece in range(2):
                self.hop(s, stage, piece, None).wait_send()


def _norm(g, gain_ref):
    step = 16
    per = g.shape[1] // step
    gain = gain_ref[...].astype(jnp.float32)

    def body(i, _):
        at = pl.ds(pl.multiple_of(lax.rem(i, per) * step, step), step)
        t = g[lax.div(i, per), at, :].astype(jnp.float32)
        scale = lax.rsqrt(jnp.mean(t * t, -1, keepdims=True) + 1e-6)
        g[lax.div(i, per), at, :] = (t * scale * gain).astype(g.dtype)

    lax.fori_loop(0, 2 * per, body, None)


def _mlp(n, h_ref, gain_ref, gate_ref, up_ref, down_ref, y_ref, g, swapped, direct, passed, near, hid, wgu, wd,
         g_send, g_recv, swap_send, swap_recv, hop_send, hop_recv, w_sem, io_sem, out_sem):
    around = _around(n)
    gather = Gather(g, g_send, g_recv, around)
    scatter = Scatter(g, swapped, direct, passed, near, (swap_send, swap_recv, hop_send, hop_recv), around)
    rows = 2 * g.shape[1]
    depth = g.shape[2]
    units = gate_ref.shape[1]
    tiles, steps = units // HIDE, scatter.steps

    def fetch(i, slot):
        at = pl.ds(pl.multiple_of(i * HIDE, HIDE), HIDE)
        return [pltpu.make_async_copy(ref.at[:, at], wgu.at[slot, k], w_sem.at[slot * 2 + k]) for k, ref in enumerate((gate_ref, up_ref))]

    def fetch_down(i, slot):
        return pltpu.make_async_copy(down_ref.at[:, scatter.cols(i)], wd.at[slot], w_sem.at[4 + slot])

    def hidden(s, place, more):
        def body(i, _):
            slot = lax.rem(i, 2)

            @pl.when(i + 1 < tiles)
            def _():
                for c in fetch(i + 1, 1 - slot):
                    c.start()

            for c in fetch(i, slot):
                c.wait()
            at = pl.ds(pl.multiple_of(i * HIDE, HIDE), HIDE)
            for part in range(2):
                t = g[4 * s + 2 * part : 4 * s + 2 * part + 2].reshape(rows, depth)
                gate = jnp.dot(t, wgu[slot, 0], preferred_element_type=jnp.float32)
                up = jnp.dot(t, wgu[slot, 1], preferred_element_type=jnp.float32)
                hid[place, part * rows : (part + 1) * rows, at] = (gate / (1 + jnp.exp(-gate)) * up).astype(hid.dtype)

        lax.fori_loop(0, tiles, body, None)
        if more:
            for c in fetch(0, 0):
                c.start()

    def down(place, part, more=True):
        def term(i):
            slot = lax.rem(i, 2)

            @pl.when(i + 1 < steps)
            def _():
                fetch_down(i + 1, 1 - slot).start()

            fetch_down(i, slot).wait()
            t = jnp.dot(hid[place, part * rows : (part + 1) * rows, :], wd[slot], preferred_element_type=jnp.float32)
            return t

        return term

    def again():
        fetch_down(0, 0).start()

    load = pltpu.make_async_copy(h_ref, g.at[pl.ds(0, 2)], io_sem.at[0])
    load.start()
    for c in fetch(0, 0):
        c.start()
    again()
    _enter(*around)
    load.wait()
    _norm(g, gain_ref)
    gather.start(4, 5, 2, 3, 9, 8)
    gather.arrived(2, 3)
    hidden(OWN, 1, True)
    gather.arrived(4, 5)
    gather.start(12, 13, 6, 7)
    gather.arrived(6, 7)
    hidden(FIRST, 0, True)
    gather.sent(4, 5, 2, 3, 9, 8)
    scatter.others(FIRST, 2, down(0, 1))
    again()
    gather.arrived(8, 9)
    gather.start(10, 11)
    scatter.mine(FIRST, 0, down(0, 0))
    again()
    gather.arrived(10, 11)
    hidden(SECOND, 2, True)
    gather.arrived(12, 13)
    gather.start(14, 15)
    gather.arrived(14, 15)
    hidden(FAR, 0, False)
    gather.sent(12, 13, 6, 7, 10, 11, 14, 15)
    load = pltpu.make_async_copy(h_ref, g.at[pl.ds(12, 2)], io_sem.at[0])
    load.start()
    scatter.others(FAR, 6, down(0, 1))
    again()
    scatter.mine(FAR, 4, down(0, 0))
    again()
    scatter.others(SECOND, 10, down(2, 1))
    again()
    scatter.mine(SECOND, 8, down(2, 0))
    again()
    scatter.others(OWN, 14, down(1, 1))
    again()
    load.wait()
    scatter.finish(12, down(1, 0), y_ref, out_sem)
    scatter.sent()


def _buffers(half, depth):
    piece = lambda k: pltpu.VMEM((k, half, depth), jnp.bfloat16)
    steps = depth // COLS
    buffers = [piece(16), pltpu.VMEM((4, 2, half, depth), jnp.bfloat16), piece(2), piece(2), piece(2)]
    sems = [pltpu.SemaphoreType.DMA((k,)) for k in (16, 16, 4, 4 * steps, 6, 6 * steps)]
    return buffers, sems


def mlp(n, h, gain, gate, up, down):
    rows, depth = h.shape
    half = rows // 2
    units = gate.shape[1]
    buffers, sems = _buffers(half, depth)
    any_space = pl.BlockSpec(memory_space=pl.ANY)
    y = pl.pallas_call(
        functools.partial(_mlp, n),
        out_shape=jax.ShapeDtypeStruct((2, half, depth), h.dtype),
        in_specs=[any_space, pl.BlockSpec(memory_space=pltpu.VMEM), any_space, any_space, any_space],
        out_specs=any_space,
        scratch_shapes=[*buffers, pltpu.VMEM((3, 2 * rows, units), h.dtype), pltpu.VMEM((2, 2, depth, HIDE), h.dtype),
                        pltpu.VMEM((2, units, COLS), h.dtype), *sems, pltpu.SemaphoreType.DMA((6,)), pltpu.SemaphoreType.DMA((1,)),
                        pltpu.SemaphoreType.DMA((2 * depth // COLS,))],
        compiler_params=pltpu.CompilerParams(collective_id=1, has_side_effects=True, vmem_limit_bytes=FULL),
        cost_estimate=pl.CostEstimate(flops=6 * rows * n * depth * units, transcendentals=rows * n * units,
                                      bytes_accessed=12 * depth * units),
    )(h.reshape(2, half, depth), gain.reshape(1, depth), gate, up, down)
    return y.reshape(rows, depth)


def _turned(t, cos, sin):
    half = HEAD // 2
    t = t.astype(jnp.bfloat16).astype(jnp.float32)
    a, b = t[:, :half], t[:, half:]
    return jnp.concatenate([a * cos - b * sin, b * cos + a * sin], -1).astype(jnp.bfloat16)


def _attention(n, x_ref, gain_ref, frequency_ref, wq_ref, wk_ref, wv_ref, wo_ref, y_ref, g, swapped, direct, passed, near, w, wo, queries, kv,
               seen, top_s, mix_s, cos_s, sin_s, cos0_s, sin0_s, g_send, g_recv, swap_send, swap_recv, hop_send, hop_recv, w_sem, io_sem, out_sem):
    around = _around(n)
    gather = Gather(g, g_send, g_recv, around)
    scatter = Scatter(g, swapped, direct, passed, near, (swap_send, swap_recv, hop_send, hop_recv), around)
    half, depth = g.shape[1], g.shape[2]
    rows = 2 * half
    heads = wq_ref.shape[1] // HEAD
    cols = 2 * heads * half
    me = lax.axis_index("tp")
    core = lax.rem(me, 2)
    e = HEAD**-0.5 * LOG2E

    def chip(shift):
        return lax.rem(me - core + 2 * shift + n, n)

    SHIFT = {OWN: (0, 0), FIRST: (-1, 1), SECOND: (1, -1), FAR: (2, 2)}

    def number(s, pair):
        a, b = SHIFT[s]
        return 2 * (chip(a) * (1 - pair) + chip(b) * pair) + pair

    copies = [pltpu.make_async_copy(ref, w.at[:, pl.ds(at, ref.shape[1])], w_sem.at[k])
              for k, (ref, at) in enumerate(((wq_ref, 0), (wk_ref, heads * HEAD), (wv_ref, (heads + 1) * HEAD)))]
    copies.append(pltpu.make_async_copy(wo_ref, wo, w_sem.at[3]))

    def project(s, part, columns):
        t = g[4 * s + 2 * part : 4 * s + 2 * part + 2].reshape(rows, depth)
        for c in columns:
            r = jnp.dot(t, w[:, c * HEAD : (c + 1) * HEAD], preferred_element_type=jnp.float32)
            for pair in range(2):
                piece = number(s, pair) + 2 * (core + part - 2 * core * part)
                z = r[pair * half : (pair + 1) * half]
                at = pl.ds(pl.multiple_of(piece * half, 64), half)
                if c == heads + 1:
                    kv[at, HEAD:] = z.astype(jnp.bfloat16)
                    continue
                c0, s0 = cos0_s[pl.ds(piece, 1), :], sin0_s[pl.ds(piece, 1), :]
                z = _turned(z, cos_s[...] * c0 - sin_s[...] * s0, sin_s[...] * c0 + cos_s[...] * s0)
                if c == heads:
                    kv[at, :HEAD] = z
                else:
                    queries[2 * s + pair, (part * heads + c) * half : (part * heads + c + 1) * half, :] = z

    def begin(pair):
        top_s[pair] = jnp.full((1, cols), NEG, jnp.float32)
        mix_s[pair] = jnp.zeros((HEAD + 8, cols), jnp.float32)

    def attend(s, pair, first, end):
        lowest = number(s, pair) * half
        column = lax.broadcasted_iota(jnp.int32, (1, cols), 1)
        behind = jnp.where(column < heads * half, core * rows, (1 - core) * rows)
        place = lax.rem(column, half) + behind + lowest
        ones = jnp.ones((8, BK), jnp.bfloat16)

        def block(j, masked):
            here = pl.ds(pl.multiple_of(j * BK, BK), BK)
            keys = kv[here, :HEAD]
            values = jnp.concatenate([kv[here, HEAD:].T, ones], axis=0)
            strips = range(0, cols, WIDE)
            scores = [_dot(keys, queries[2 * s + pair, at : at + WIDE, :], 1, 1) for at in strips]
            weights, keeps = [], []
            for at, z in zip(strips, scores):
                if masked:
                    key = lax.broadcasted_iota(jnp.int32, z.shape, 0) + j * BK
                    z = jnp.where(key <= place[:, at : at + WIDE], z, HIDDEN)
                old = top_s[pair, :, at : at + WIDE]
                top = jnp.maximum(old, z.max(axis=0, keepdims=True))
                top_s[pair, :, at : at + WIDE] = top
                weights.append(jnp.exp2((z - top) * e).astype(jnp.bfloat16))
                keeps.append(jnp.exp2((old - top) * e))
            for at, p, keep in zip(strips, weights, keeps):
                mix_s[pair, :, at : at + WIDE] = mix_s[pair, :, at : at + WIDE] * keep + _dot(values, p, 1, 0)

        whole = lax.div(lowest + 1, BK)
        last = lax.div(lowest + rows + half + BK - 1, BK)
        whole = jnp.minimum(jnp.maximum(whole, first), end)
        last = jnp.minimum(jnp.maximum(last, first), end)
        lax.fori_loop(first, whole, lambda j, _: block(j, False), None)
        lax.fori_loop(whole, last, lambda j, _: block(j, True), None)

    def done(pair):
        out = (mix_s[pair, :HEAD, :] * (1 / mix_s[pair, HEAD : HEAD + 1, :])).T.astype(jnp.bfloat16)
        for part in range(2):
            for h in range(heads):
                at = (part * heads + h) * half
                seen[2 * part + pair, :, h * HEAD : (h + 1) * HEAD] = out[at : at + half, :]

    def pairs(body):
        lax.fori_loop(0, 2, lambda pair, _: body(pair), None)

    def attended(s):
        def body(pair):
            begin(pair)
            attend(s, pair, 0, kv.shape[0] // BK)
            done(pair)

        pairs(body)

    def some(s, shift):
        per = 2 * rows // BK
        first = lax.div(chip(shift), 2) * per
        pairs(lambda pair: attend(s, pair, first, first + per))

    def result(part):
        def term(i):
            return jnp.dot(seen[2 * part : 2 * part + 2].reshape(rows, heads * HEAD), wo[:, scatter.cols(i)], preferred_element_type=jnp.float32)

        return term

    load = pltpu.make_async_copy(x_ref, g.at[pl.ds(0, 2)], io_sem.at[0])
    load.start()
    _enter(*around)
    load.wait()
    _norm(g, gain_ref)
    gather.start(4, 5, 2, 3, 9, 8)
    for c in copies:
        c.start()
    angle = lax.broadcasted_iota(jnp.int32, cos_s.shape, 0).astype(jnp.float32) * frequency_ref[...]
    cos_s[...], sin_s[...] = jnp.cos(angle), jnp.sin(angle)
    angle = (lax.broadcasted_iota(jnp.int32, cos0_s.shape, 0) * half).astype(jnp.float32) * frequency_ref[...]
    cos0_s[...], sin0_s[...] = jnp.cos(angle), jnp.sin(angle)
    for c in copies:
        c.wait()
    every, q_columns, kv_columns = range(heads + 2), range(heads), range(heads, heads + 2)
    project(OWN, 0, every)
    gather.arrived(2, 3)
    project(OWN, 1, every)
    gather.arrived(4, 5)
    gather.start(12, 13, 6, 7)
    project(FIRST, 0, every)
    gather.arrived(6, 7)
    project(FIRST, 1, every)
    gather.arrived(8, 9)
    gather.start(10, 11)
    project(SECOND, 0, every)
    gather.arrived(10, 11)
    project(SECOND, 1, every)
    pairs(begin)
    for shift in (0, 1, -1):
        some(FIRST, shift)
    gather.sent(4, 5, 2, 3, 9, 8)
    gather.arrived(12, 13)
    gather.start(14, 15)
    project(FAR, 0, kv_columns)
    gather.arrived(14, 15)
    project(FAR, 1, kv_columns)
    some(FIRST, 2)
    pairs(done)
    scatter.others(FIRST, 2, result(1))
    scatter.mine(FIRST, 0, result(0))
    project(FAR, 0, q_columns)
    project(FAR, 1, q_columns)
    gather.sent(12, 13, 6, 7, 10, 11, 14, 15)
    load = pltpu.make_async_copy(x_ref, g.at[pl.ds(12, 2)], io_sem.at[0])
    load.start()
    attended(FAR)
    scatter.others(FAR, 6, result(1))
    scatter.mine(FAR, 4, result(0))
    attended(SECOND)
    scatter.others(SECOND, 10, result(1))
    scatter.mine(SECOND, 8, result(0))
    attended(OWN)
    scatter.others(OWN, 14, result(1))
    load.wait()
    scatter.finish(12, result(0), y_ref, out_sem)
    scatter.sent()


def attention(n, x, gain, wq, wk, wv, wo):
    rows, depth = x.shape
    half = rows // 2
    heads = wq.shape[1] // HEAD
    cols = 2 * heads * half
    buffers, sems = _buffers(half, depth)
    any_space, vmem = pl.BlockSpec(memory_space=pl.ANY), pl.BlockSpec(memory_space=pltpu.VMEM)
    frequency = THETA ** (-jnp.arange(HEAD // 2, dtype=jnp.float32) / (HEAD // 2))
    trig = [pltpu.VMEM((k, HEAD // 2), jnp.float32) for k in (half, half, 2 * n, 2 * n)]
    y = pl.pallas_call(
        functools.partial(_attention, n),
        out_shape=jax.ShapeDtypeStruct((2, half, depth), x.dtype),
        in_specs=[any_space, vmem, vmem, any_space, any_space, any_space, any_space],
        out_specs=any_space,
        scratch_shapes=[*buffers, pltpu.VMEM((depth, (heads + 2) * HEAD), x.dtype), pltpu.VMEM((heads * HEAD, depth), x.dtype),
                        pltpu.VMEM((8, cols, HEAD), x.dtype), pltpu.VMEM((n * rows, 2 * HEAD), x.dtype),
                        pltpu.VMEM((4, half, heads * HEAD), x.dtype), pltpu.VMEM((2, 1, cols), jnp.float32),
                        pltpu.VMEM((2, HEAD + 8, cols), jnp.float32), *trig, *sems, pltpu.SemaphoreType.DMA((4,)),
                        pltpu.SemaphoreType.DMA((1,)), pltpu.SemaphoreType.DMA((2 * depth // COLS,))],
        compiler_params=pltpu.CompilerParams(collective_id=0, has_side_effects=True, vmem_limit_bytes=FULL),
        cost_estimate=pl.CostEstimate(flops=2 * rows * n * depth * (2 * heads + 2) * HEAD, transcendentals=rows * n * rows * n,
                                      bytes_accessed=4 * depth * (2 * heads + 2) * HEAD),
    )(x.reshape(2, half, depth), gain.reshape(1, depth), frequency.reshape(1, -1), wq, wk, wv, wo)
    return y.reshape(rows, depth)


def solution(mesh):
    n = mesh.shape["tp"]

    def step(x, gain_a, wq, wk, wv, wo, gain_m, w_gate, w_up, w_down):
        h = attention(n, x, gain_a, wq, wk, wv, wo)
        return mlp(n, h, gain_m, w_gate, w_up, w_down)

    tokens, columns, rows_of = P(("dp", "tp"), None), P(None, "tp"), P("tp", None)
    return jax.shard_map(
        step,
        mesh=mesh,
        in_specs=(tokens, P(None), columns, columns, columns, rows_of, P(None), columns, columns, rows_of),
        out_specs=tokens,
        check_vma=False,
    )
```

```python
import functools
import math

import jax
import jax.numpy as jnp
from jax import lax
from jax.experimental import pallas as pl
from jax.experimental.pallas import tpu as pltpu
from jax.sharding import PartitionSpec as P

NEG = -1e30
HIDDEN = 2 * NEG
LOG2E = 1.4426950408889634
HEAD = 256
THETA = 10000
BK = 256
WIDE = 256


def _dot(a, b, ca, cb):
    return lax.dot_general(a, b, (((ca,), (cb,)), ((), ())), preferred_element_type=jnp.float32)


MESH = pl.DeviceIdType.MESH
FULL = 67_043_328
COLS = 512
HIDE = 256
OWN, FIRST, SECOND, FAR = range(4)


def _around(n):
    me = lax.axis_index("tp")
    return lax.rem(me + 2, n), lax.rem(me + n - 2, n), me + 1 - 2 * lax.rem(me, 2)


def _enter(*others):
    barrier = pltpu.get_barrier_semaphore()
    for other in others:
        pl.semaphore_signal(barrier, inc=1, device_id={"tp": other}, device_id_type=MESH)
    pl.semaphore_wait(barrier, len(others))


class Gather:
    def __init__(self, g, send, recv, around):
        self.g, self.sems, self.around = g, (send, recv), around

    PATH = {4: (0, "right"), 5: (1, "left"), 9: (1, "right"), 8: (0, "left"), 12: (4, "right"), 13: (5, "left"),
            2: (0, "twin"), 3: (1, "twin"), 6: (4, "twin"), 7: (5, "twin"), 10: (8, "twin"), 11: (9, "twin"), 14: (12, "twin"), 15: (13, "twin")}

    def copies(self, slots, sub):
        right, left, twin = self.around
        rows = self.g.shape[1]
        at = pl.ds(0, rows) if sub is None else pl.ds(sub * (rows // 2), rows // 2)
        made = []
        for slot in slots:
            source, to = self.PATH[slot]
            sem = slot + (4 if sub == 1 else 0)
            made.append(pltpu.make_async_remote_copy(
                src_ref=self.g.at[source, at], dst_ref=self.g.at[slot, at], send_sem=self.sems[0].at[sem], recv_sem=self.sems[1].at[sem],
                device_id={"tp": {"right": right, "left": left, "twin": twin}[to]}, device_id_type=MESH))
        return made

    def start(self, *slots, sub=None):
        for c in self.copies(slots, sub):
            c.start()

    def arrived(self, *slots, sub=None):
        for c in self.copies(slots, sub):
            c.wait_recv()

    def sent(self, *slots, sub=None):
        for c in self.copies(slots, sub):
            c.wait_send()


class Scatter:
    def __init__(self, g, swapped, direct, passed, near, sems, around):
        self.g, self.swapped, self.direct, self.passed, self.near, self.around = g, swapped, direct, passed, near, around
        self.swap_send, self.swap_recv, self.send, self.recv = sems
        self.steps = g.shape[2] // COLS
        self.quarter = g.shape[1] // 2

    def cols(self, n):
        return pl.ds(0, self.g.shape[2]) if n is None else pl.ds(pl.multiple_of(n * COLS, COLS), COLS)

    def rows(self, sub):
        return pl.ds(0, 2 * self.quarter) if sub is None else pl.ds(sub * self.quarter, self.quarter)

    def parts(self, sub):
        subs = range(2) if sub is None else (sub,)
        return [(slice((2 * i + piece) * self.quarter, (2 * i + piece + 1) * self.quarter), piece, self.rows(k))
                for i, k in enumerate(subs) for piece in range(2)]

    def swap(self, s, stage, n, sub):
        k = 4 if sub == 1 else s
        return pltpu.make_async_remote_copy(
            src_ref=self.g.at[pl.ds(stage, 2), self.rows(sub), self.cols(n)], dst_ref=self.swapped.at[s, :, self.rows(sub), self.cols(n)],
            send_sem=self.swap_send.at[k], recv_sem=self.swap_recv.at[k * self.steps + (0 if n is None else n)],
            device_id={"tp": self.around[2]}, device_id_type=MESH)

    def hop(self, s, stage, piece, n, sub):
        right, left, _ = self.around
        to = left if (s == FIRST) == (piece == 0) else right
        buffer = {FIRST: self.direct, FAR: self.passed, SECOND: self.near}[s]
        k = ({FIRST: 0, FAR: 1, SECOND: 2}[s] + (2 if sub == 1 else 0)) * 2 + piece
        return pltpu.make_async_remote_copy(
            src_ref=self.g.at[stage + piece, self.rows(sub), self.cols(n)], dst_ref=buffer.at[piece, self.rows(sub), self.cols(n)],
            send_sem=self.send.at[k], recv_sem=self.recv.at[k * self.steps + (0 if n is None else n)],
            device_id={"tp": to}, device_id_type=MESH)

    def others(self, s, stage, term, sub=None):
        def body(n, _):
            t = term(n)
            for at, piece, rows in self.parts(sub):
                self.g[stage + piece, rows, self.cols(n)] = t[at].astype(self.g.dtype)

            @pl.when(n > 0)
            def _():
                self.swap(s, stage, n - 1, sub).start()

        lax.fori_loop(0, self.steps, body, None)
        self.swap(s, stage, self.steps - 1, sub).start()

    def mine(self, s, stage, term, sub=None, passed=()):
        def body(n, _):
            t = term(n)
            self.swap(s, stage, n, sub).wait_recv()
            for k in passed:
                for piece in range(2):
                    self.hop(FAR, stage, piece, n, k).wait_recv()
            for at, piece, rows in self.parts(sub):
                total = t[at] + self.swapped[s, piece, rows, self.cols(n)].astype(jnp.float32)
                if passed:
                    total += self.passed[piece, rows, self.cols(n)].astype(jnp.float32)
                self.g[stage + piece, rows, self.cols(n)] = total.astype(self.g.dtype)

            @pl.when(n > 0)
            def _():
                for piece in range(2):
                    self.hop(s, stage, piece, n - 1, sub).start()

        lax.fori_loop(0, self.steps, body, None)
        for piece in range(2):
            self.hop(s, stage, piece, self.steps - 1, sub).start()

    def finish(self, stage, term, out, out_sem):
        def whole(n, piece):
            return pltpu.make_async_copy(self.g.at[stage + piece, :, self.cols(n)], out.at[piece, :, self.cols(n)], out_sem.at[n * 2 + piece])

        def early(n, _):
            for piece in range(2):
                self.hop(FIRST, stage, piece, n, None).wait_recv()

        lax.fori_loop(0, self.steps, early, None)

        def body(n, _):
            t = term(n)
            self.swap(OWN, stage, n, None).wait_recv()
            for piece in range(2):
                self.hop(SECOND, stage, piece, n, None).wait_recv()
            for at, piece, rows in self.parts(None):
                total = t[at] + self.swapped[OWN, piece, rows, self.cols(n)].astype(jnp.float32)
                total += self.direct[piece, rows, self.cols(n)].astype(jnp.float32)
                total += self.near[piece, rows, self.cols(n)].astype(jnp.float32)
                total += self.g[stage + piece, rows, self.cols(n)].astype(jnp.float32)
                self.g[stage + piece, rows, self.cols(n)] = total.astype(self.g.dtype)

            @pl.when(n > 0)
            def _():
                for piece in range(2):
                    whole(n - 1, piece).start()

        lax.fori_loop(0, self.steps, body, None)
        for piece in range(2):
            whole(self.steps - 1, piece).start()

        def end(n, _):
            for piece in range(2):
                whole(n, piece).wait()

        lax.fori_loop(0, self.steps, end, None)

    def sent(self, far_subs):
        for s, stage, subs in ((FIRST, 2, (None,)), (FAR, 6, far_subs), (SECOND, 10, (None,)), (OWN, 14, (None,))):
            for sub in subs:
                self.swap(s, stage, None, sub).wait_send()
        for s, stage, subs in ((FIRST, 0, (None,)), (FAR, 4, far_subs), (SECOND, 8, (None,))):
            for sub in subs:
                for piece in range(2):
                    self.hop(s, stage, piece, None, sub).wait_send()


def _norm(g, gain_ref):
    step = 16
    per = g.shape[1] // step
    gain = gain_ref[...].reshape(1, -1).astype(jnp.float32)

    def body(i, _):
        at = pl.ds(pl.multiple_of(lax.rem(i, per) * step, step), step)
        t = g[lax.div(i, per), at, :].astype(jnp.float32)
        scale = lax.rsqrt(jnp.mean(t * t, -1, keepdims=True) + 1e-6)
        g[lax.div(i, per), at, :] = (t * scale * gain).astype(g.dtype)

    lax.fori_loop(0, 2 * per, body, None)


def _mlp(n, h_ref, gain_ref, gate_ref, up_ref, down_ref, y_ref, g, swapped, direct, passed, near, hid, wgu, wd,
         g_send, g_recv, swap_send, swap_recv, hop_send, hop_recv, w_sem, io_sem, out_sem):
    around = _around(n)
    gather = Gather(g, g_send, g_recv, around)
    scatter = Scatter(g, swapped, direct, passed, near, (swap_send, swap_recv, hop_send, hop_recv), around)
    rows = 2 * g.shape[1]
    depth = g.shape[2]
    units = gate_ref.shape[1]
    tiles, steps = units // HIDE, scatter.steps

    def fetch(i, slot):
        at = pl.ds(pl.multiple_of(i * HIDE, HIDE), HIDE)
        return [pltpu.make_async_copy(ref.at[:, at], wgu.at[slot, k], w_sem.at[slot * 2 + k]) for k, ref in enumerate((gate_ref, up_ref))]

    def fetch_down(i, slot):
        return pltpu.make_async_copy(down_ref.at[:, scatter.cols(i)], wd.at[slot], w_sem.at[4 + slot])

    quarter = scatter.quarter

    def hidden(s, place, subs, more=True):
        def body(i, _):
            slot = lax.rem(i, 2)

            @pl.when(i + 1 < tiles)
            def _():
                for c in fetch(i + 1, 1 - slot):
                    c.start()

            for c in fetch(i, slot):
                c.wait()
            at = pl.ds(pl.multiple_of(i * HIDE, HIDE), HIDE)
            for sub in subs:
                t = g[4 * s : 4 * s + 4, scatter.rows(sub), :].reshape(rows, depth)
                gate = jnp.dot(t, wgu[slot, 0], preferred_element_type=jnp.float32)
                up = jnp.dot(t, wgu[slot, 1], preferred_element_type=jnp.float32)
                hid[place, sub * rows : (sub + 1) * rows, at] = (gate / (1 + jnp.exp(-gate)) * up).astype(hid.dtype)

        lax.fori_loop(0, tiles, body, None)
        if more:
            for c in fetch(0, 0):
                c.start()

    def down(place, part, subs=(0, 1)):
        def term(i):
            slot = lax.rem(i, 2)

            @pl.when(i + 1 < steps)
            def _():
                fetch_down(i + 1, 1 - slot).start()

            fetch_down(i, slot).wait()
            t = [hid[place, (4 * sub + 2 * part) * quarter : (4 * sub + 2 * part + 2) * quarter, :] for sub in subs]
            return jnp.dot(jnp.concatenate(t, 0), wd[slot], preferred_element_type=jnp.float32)

        return term

    def again():
        fetch_down(0, 0).start()

    def far(sub):
        gather.arrived(12, 13, sub=sub)
        gather.start(14, 15, sub=sub)
        gather.arrived(14, 15, sub=sub)

    load = pltpu.make_async_copy(h_ref, g.at[pl.ds(0, 2)], io_sem.at[0])
    load.start()
    for c in fetch(0, 0):
        c.start()
    again()
    _enter(*around)
    load.wait()
    _norm(g, gain_ref)
    gather.start(4, 5, 2, 3, 9, 8)
    gather.arrived(2, 3)
    hidden(OWN, 1, (0, 1))
    gather.arrived(4, 5)
    gather.start(12, 13, sub=0)
    gather.start(12, 13, sub=1)
    gather.start(6, 7)
    gather.arrived(6, 7)
    hidden(FIRST, 0, (0, 1))
    gather.sent(4, 5, 2, 3, 9, 8)
    scatter.others(FIRST, 2, down(0, 1))
    again()
    gather.arrived(8, 9)
    gather.start(10, 11)
    scatter.mine(FIRST, 0, down(0, 0))
    again()
    far(0)
    hidden(FAR, 0, (0,))
    gather.sent(12, 13, sub=0)
    gather.sent(12, 13, sub=1)
    gather.sent(6, 7)
    scatter.others(FAR, 6, down(0, 1, (0,)), 0)
    again()
    scatter.mine(FAR, 4, down(0, 0, (0,)), 0)
    again()
    gather.arrived(10, 11)
    hidden(SECOND, 2, (0,))
    far(1)
    hidden(FAR, 0, (1,))
    scatter.others(FAR, 6, down(0, 1, (1,)), 1)
    again()
    scatter.mine(FAR, 4, down(0, 0, (1,)), 1)
    again()
    hidden(SECOND, 2, (1,), False)
    gather.sent(10, 11)
    gather.sent(14, 15, sub=0)
    gather.sent(14, 15, sub=1)
    load = pltpu.make_async_copy(h_ref, g.at[pl.ds(12, 2)], io_sem.at[0])
    load.start()
    scatter.others(SECOND, 10, down(2, 1))
    again()
    scatter.mine(SECOND, 8, down(2, 0), passed=(0, 1))
    again()
    scatter.others(OWN, 14, down(1, 1))
    again()
    load.wait()
    scatter.finish(12, down(1, 0), y_ref, out_sem)
    scatter.sent((0, 1))


def _buffers(half, depth):
    piece = lambda k: pltpu.VMEM((k, half, depth), jnp.bfloat16)
    steps = depth // COLS
    buffers = [piece(16), pltpu.VMEM((4, 2, half, depth), jnp.bfloat16), piece(2), piece(2), piece(2)]
    sems = [pltpu.SemaphoreType.DMA((k,)) for k in (20, 20, 5, 5 * steps, 8, 8 * steps)]
    return buffers, sems


def mlp(n, h, gain, gate, up, down):
    rows, depth = h.shape
    half = rows // 2
    units = gate.shape[1]
    buffers, sems = _buffers(half, depth)
    any_space = pl.BlockSpec(memory_space=pl.ANY)
    y = pl.pallas_call(
        functools.partial(_mlp, n),
        out_shape=jax.ShapeDtypeStruct((2, half, depth), h.dtype),
        in_specs=[any_space, pl.BlockSpec(memory_space=pltpu.VMEM), any_space, any_space, any_space],
        out_specs=any_space,
        scratch_shapes=[*buffers, pltpu.VMEM((3, 2 * rows, units), h.dtype), pltpu.VMEM((2, 2, depth, HIDE), h.dtype),
                        pltpu.VMEM((2, units, COLS), h.dtype), *sems, pltpu.SemaphoreType.DMA((6,)), pltpu.SemaphoreType.DMA((1,)),
                        pltpu.SemaphoreType.DMA((2 * depth // COLS,))],
        compiler_params=pltpu.CompilerParams(collective_id=1, has_side_effects=True, vmem_limit_bytes=FULL),
        cost_estimate=pl.CostEstimate(flops=6 * rows * n * depth * units, transcendentals=rows * n * units,
                                      bytes_accessed=12 * depth * units),
    )(h.reshape(2, half, depth), gain, gate, up, down)
    return y.reshape(rows, depth)


def _turned(t, cos, sin):
    half = HEAD // 2
    t = t.astype(jnp.bfloat16).astype(jnp.float32)
    a, b = t[:, :half], t[:, half:]
    return jnp.concatenate([a * cos - b * sin, b * cos + a * sin], -1).astype(jnp.bfloat16)


def _attention(n, x_ref, gain_ref, wq_ref, wk_ref, wv_ref, wo_ref, y_ref, g, swapped, direct, passed, near, w, wo, queries, kv,
               seen, top_s, mix_s, cos_s, sin_s, cos0_s, sin0_s, g_send, g_recv, swap_send, swap_recv, hop_send, hop_recv, w_sem, io_sem, out_sem):
    around = _around(n)
    gather = Gather(g, g_send, g_recv, around)
    scatter = Scatter(g, swapped, direct, passed, near, (swap_send, swap_recv, hop_send, hop_recv), around)
    half, depth = g.shape[1], g.shape[2]
    rows = 2 * half
    heads = wq_ref.shape[1] // HEAD
    cols = 2 * heads * half
    me = lax.axis_index("tp")
    core = lax.rem(me, 2)
    e = HEAD**-0.5 * LOG2E

    def chip(shift):
        return lax.rem(me - core + 2 * shift + n, n)

    def number(s, pair):
        shift = jnp.where(s == FIRST, 2 * pair - 1, jnp.where(s == SECOND, 1 - 2 * pair, jnp.where(s == FAR, 2, 0)))
        return 2 * chip(shift) + pair

    copies = [pltpu.make_async_copy(ref, w.at[:, pl.ds(at, ref.shape[1])], w_sem.at[k])
              for k, (ref, at) in enumerate(((wq_ref, 0), (wk_ref, heads * HEAD), (wv_ref, (heads + 1) * HEAD)))]
    copies.append(pltpu.make_async_copy(wo_ref, wo, w_sem.at[3]))

    def project(s, part, columns, sub=None):
        size = half if sub is None else half // 2
        start = (sub or 0) * size
        t = g[pl.ds(4 * s + 2 * part, 2), start : start + size, :].reshape(2 * size, depth)
        for c in columns:
            r = jnp.dot(t, w[:, c * HEAD : (c + 1) * HEAD], preferred_element_type=jnp.float32)
            for pair in range(2):
                piece = number(s, pair) + 2 * (core + part - 2 * core * part)
                z = r[pair * size : (pair + 1) * size]
                at = pl.ds(pl.multiple_of(piece * half + start, 32), size)
                if c == heads + 1:
                    kv[at, HEAD:] = z.astype(jnp.bfloat16)
                    continue
                c0, s0 = cos0_s[pl.ds(piece, 1), :], sin0_s[pl.ds(piece, 1), :]
                cos, sin = cos_s[start : start + size, :], sin_s[start : start + size, :]
                z = _turned(z, cos * c0 - sin * s0, sin * c0 + cos * s0)
                if c == heads:
                    kv[at, :HEAD] = z
                else:
                    queries[2 * s + pair, pl.ds(pl.multiple_of((part * heads + c) * half + start, 32), size), :] = z

    def begin(pair):
        top_s[pair] = jnp.full((1, cols), NEG, jnp.float32)
        mix_s[pair] = jnp.zeros((HEAD + 8, cols), jnp.float32)

    def attend(s, pair, first, end):
        lowest = number(s, pair) * half
        column = lax.broadcasted_iota(jnp.int32, (1, cols), 1)
        behind = jnp.where(column < heads * half, core * rows, (1 - core) * rows)
        place = lax.rem(column, half) + behind + lowest
        ones = jnp.ones((8, BK), jnp.bfloat16)

        def block(j, masked):
            here = pl.ds(pl.multiple_of(j * BK, BK), BK)
            keys = kv[here, :HEAD]
            values = jnp.concatenate([kv[here, HEAD:].T, ones], axis=0)
            strips = range(0, cols, WIDE)
            scores = [_dot(keys, queries[2 * s + pair, at : at + WIDE, :], 1, 1) for at in strips]
            weights, keeps = [], []
            for at, z in zip(strips, scores):
                if masked:
                    key = lax.broadcasted_iota(jnp.int32, z.shape, 0) + j * BK
                    z = jnp.where(key <= place[:, at : at + WIDE], z, HIDDEN)
                old = top_s[pair, :, at : at + WIDE]
                top = jnp.maximum(old, z.max(axis=0, keepdims=True))
                top_s[pair, :, at : at + WIDE] = top
                weights.append(jnp.exp2((z - top) * e).astype(jnp.bfloat16))
                keeps.append(jnp.exp2((old - top) * e))
            for at, p, keep in zip(strips, weights, keeps):
                mix_s[pair, :, at : at + WIDE] = mix_s[pair, :, at : at + WIDE] * keep + _dot(values, p, 1, 0)

        whole = lax.div(lowest + 1, BK)
        last = lax.div(lowest + rows + half + BK - 1, BK)
        whole = jnp.minimum(jnp.maximum(whole, first), end)
        last = jnp.minimum(jnp.maximum(last, first), end)
        lax.fori_loop(first, whole, lambda j, _: block(j, False), None)
        lax.fori_loop(whole, last, lambda j, _: block(j, True), None)

    def done(pair):
        out = (mix_s[pair, :HEAD, :] * (1 / mix_s[pair, HEAD : HEAD + 1, :])).T.astype(jnp.bfloat16)
        for part in range(2):
            for h in range(heads):
                at = (part * heads + h) * half
                seen[2 * part + pair, :, h * HEAD : (h + 1) * HEAD] = out[at : at + half, :]

    def pairs(body):
        lax.fori_loop(0, 2, lambda pair, _: body(pair), None)

    def attended(s):
        def body(pair):
            begin(pair)
            attend(s, pair, 0, kv.shape[0] // BK)
            done(pair)

        pairs(body)

    def some(s, shift):
        per = 2 * rows // BK
        first = lax.div(chip(shift), 2) * per
        pairs(lambda pair: attend(s, pair, first, first + per))

    def result(part):
        def term(i):
            t = [seen[2 * part + piece, at, :] for _, piece, at in scatter.parts(None)]
            return jnp.dot(jnp.concatenate(t, 0), wo[:, scatter.cols(i)], preferred_element_type=jnp.float32)

        return term

    load = pltpu.make_async_copy(x_ref, g.at[pl.ds(0, 2)], io_sem.at[0])
    load.start()
    _enter(*around)
    load.wait()
    _norm(g, gain_ref)
    gather.start(4, 5, 2, 3, 9, 8)
    for c in copies:
        c.start()
    turn = lax.broadcasted_iota(jnp.int32, (1, HEAD // 2), 1).astype(jnp.float32) / (HEAD // 2)
    frequency = jnp.exp2(-turn * math.log2(THETA))
    angle = lax.broadcasted_iota(jnp.int32, cos_s.shape, 0).astype(jnp.float32) * frequency
    cos_s[...], sin_s[...] = jnp.cos(angle), jnp.sin(angle)
    angle = (lax.broadcasted_iota(jnp.int32, cos0_s.shape, 0) * half).astype(jnp.float32) * frequency
    cos0_s[...], sin0_s[...] = jnp.cos(angle), jnp.sin(angle)
    for c in copies:
        c.wait()
    every, q_columns, kv_columns = range(heads + 2), range(heads), range(heads, heads + 2)

    def early(i, _):
        @pl.when(i == 1)
        def _():
            gather.arrived(2, 3)

        @pl.when(i == 2)
        def _():
            gather.arrived(4, 5)
            gather.start(12, 13, sub=0)
            gather.start(12, 13, sub=1)
            gather.start(6, 7)

        @pl.when(i == 3)
        def _():
            gather.arrived(6, 7)

        @pl.when(i == 4)
        def _():
            gather.arrived(8, 9)
            gather.start(10, 11)

        @pl.when(i == 5)
        def _():
            gather.arrived(10, 11)

        project(lax.div(i, 2), lax.rem(i, 2), every)

    lax.fori_loop(0, 6, early, None)
    pairs(begin)
    lax.fori_loop(0, 3, lambda i, _: some(FIRST, i - 1), None)
    gather.sent(4, 5, 2, 3, 9, 8)
    for sub in range(2):
        gather.arrived(12, 13, sub=sub)
        gather.start(14, 15, sub=sub)
        project(FAR, 0, kv_columns, sub)
        gather.arrived(14, 15, sub=sub)
        project(FAR, 1, kv_columns, sub)
    some(FIRST, 2)
    pairs(done)
    scatter.others(FIRST, 2, result(1))
    scatter.mine(FIRST, 0, result(0))
    lax.fori_loop(0, 2, lambda part, _: project(FAR, part, q_columns), None)
    for sub in range(2):
        gather.sent(12, 13, 14, 15, sub=sub)
    gather.sent(6, 7, 10, 11)
    load = pltpu.make_async_copy(x_ref, g.at[pl.ds(12, 2)], io_sem.at[0])
    load.start()
    attended(FAR)
    scatter.others(FAR, 6, result(1))
    scatter.mine(FAR, 4, result(0))
    attended(SECOND)
    scatter.others(SECOND, 10, result(1))
    scatter.mine(SECOND, 8, result(0), passed=(None,))
    attended(OWN)
    scatter.others(OWN, 14, result(1))
    load.wait()
    scatter.finish(12, result(0), y_ref, out_sem)
    scatter.sent((None,))


def attention(n, x, gain, wq, wk, wv, wo):
    rows, depth = x.shape
    half = rows // 2
    heads = wq.shape[1] // HEAD
    cols = 2 * heads * half
    buffers, sems = _buffers(half, depth)
    any_space, vmem = pl.BlockSpec(memory_space=pl.ANY), pl.BlockSpec(memory_space=pltpu.VMEM)
    trig = [pltpu.VMEM((k, HEAD // 2), jnp.float32) for k in (half, half, 2 * n, 2 * n)]
    y = pl.pallas_call(
        functools.partial(_attention, n),
        out_shape=jax.ShapeDtypeStruct((2, half, depth), x.dtype),
        in_specs=[any_space, vmem, any_space, any_space, any_space, any_space],
        out_specs=any_space,
        scratch_shapes=[*buffers, pltpu.VMEM((depth, (heads + 2) * HEAD), x.dtype), pltpu.VMEM((heads * HEAD, depth), x.dtype),
                        pltpu.VMEM((8, cols, HEAD), x.dtype), pltpu.VMEM((n * rows, 2 * HEAD), x.dtype),
                        pltpu.VMEM((4, half, heads * HEAD), x.dtype), pltpu.VMEM((2, 1, cols), jnp.float32),
                        pltpu.VMEM((2, HEAD + 8, cols), jnp.float32), *trig, *sems, pltpu.SemaphoreType.DMA((4,)),
                        pltpu.SemaphoreType.DMA((1,)), pltpu.SemaphoreType.DMA((2 * depth // COLS,))],
        compiler_params=pltpu.CompilerParams(collective_id=0, has_side_effects=True, vmem_limit_bytes=FULL),
        cost_estimate=pl.CostEstimate(flops=2 * rows * n * depth * (2 * heads + 2) * HEAD, transcendentals=rows * n * rows * n,
                                      bytes_accessed=4 * depth * (2 * heads + 2) * HEAD),
    )(x.reshape(2, half, depth), gain, wq, wk, wv, wo)
    return y.reshape(rows, depth)


def solution(mesh):
    n = mesh.shape["tp"]

    def step(x, gain_a, wq, wk, wv, wo, gain_m, w_gate, w_up, w_down):
        h = attention(n, x, gain_a, wq, wk, wv, wo)
        return mlp(n, h, gain_m, w_gate, w_up, w_down)

    tokens, columns, rows_of = P(("dp", "tp"), None), P(None, "tp"), P("tp", None)
    return jax.shard_map(
        step,
        mesh=mesh,
        in_specs=(tokens, P(None), columns, columns, columns, rows_of, P(None), columns, columns, rows_of),
        out_specs=tokens,
        check_vma=False,
    )
```

```python
import functools
import math

import jax
import jax.numpy as jnp
from jax import lax
from jax.experimental import pallas as pl
from jax.experimental.pallas import tpu as pltpu
from jax.sharding import PartitionSpec as P

NEG = -1e30
HIDDEN = 2 * NEG
LOG2E = 1.4426950408889634
HEAD = 256
THETA = 10000
BK = 256
WIDE = 256


def _dot(a, b, ca, cb):
    return lax.dot_general(a, b, (((ca,), (cb,)), ((), ())), preferred_element_type=jnp.float32)


MESH = pl.DeviceIdType.MESH
FULL = 67_043_328
COLS = 512
HIDE = 256
OWN, FIRST, SECOND, FAR = range(4)


def _around(n):
    me = lax.axis_index("tp")
    return lax.rem(me + 2, n), lax.rem(me + n - 2, n), me + 1 - 2 * lax.rem(me, 2)


def _enter(*others):
    barrier = pltpu.get_barrier_semaphore()
    for other in others:
        pl.semaphore_signal(barrier, inc=1, device_id={"tp": other}, device_id_type=MESH)
    pl.semaphore_wait(barrier, len(others))


class Gather:
    def __init__(self, g, send, recv, around):
        self.g, self.sems, self.around = g, (send, recv), around

    PATH = {4: (0, "right"), 5: (1, "left"), 9: (1, "right"), 8: (0, "left"), 12: (4, "right"), 13: (5, "left"),
            2: (0, "twin"), 3: (1, "twin"), 6: (4, "twin"), 7: (5, "twin"), 10: (8, "twin"), 11: (9, "twin"), 14: (12, "twin"), 15: (13, "twin")}

    def copies(self, slots, sub):
        right, left, twin = self.around
        rows = self.g.shape[1]
        at = pl.ds(0, rows) if sub is None else pl.ds(sub * (rows // 2), rows // 2)
        made = []
        for slot in slots:
            source, to = self.PATH[slot]
            sem = slot + (4 if sub == 1 else 0)
            made.append(pltpu.make_async_remote_copy(
                src_ref=self.g.at[source, at], dst_ref=self.g.at[slot, at], send_sem=self.sems[0].at[sem], recv_sem=self.sems[1].at[sem],
                device_id={"tp": {"right": right, "left": left, "twin": twin}[to]}, device_id_type=MESH))
        return made

    def start(self, *slots, sub=None):
        for c in self.copies(slots, sub):
            c.start()

    def arrived(self, *slots, sub=None):
        for c in self.copies(slots, sub):
            c.wait_recv()

    def sent(self, *slots, sub=None):
        for c in self.copies(slots, sub):
            c.wait_send()


class Scatter:
    STAGE = {FIRST: (0, 2), FAR: (4, 6), SECOND: (8, 10), OWN: (12, 14)}

    def __init__(self, g, swapped, direct, passed, near, held, sems, around):
        self.g, self.swapped, self.direct, self.passed, self.near, self.held, self.around = g, swapped, direct, passed, near, held, around
        self.swap_send, self.swap_recv, self.send, self.recv = sems
        self.steps = g.shape[2] // COLS

    def cols(self, n):
        return pl.ds(0, self.g.shape[2]) if n is None else pl.ds(pl.multiple_of(n * COLS, COLS), COLS)

    def swap(self, s, n):
        return pltpu.make_async_remote_copy(
            src_ref=self.g.at[pl.ds(self.STAGE[s][1], 2), :, self.cols(n)], dst_ref=self.swapped.at[s, :, :, self.cols(n)],
            send_sem=self.swap_send.at[s], recv_sem=self.swap_recv.at[s * self.steps + (0 if n is None else n)],
            device_id={"tp": self.around[2]}, device_id_type=MESH)

    def hop(self, s, piece, n):
        right, left, _ = self.around
        to = left if (s == FIRST) == (piece == 0) else right
        buffer = {FIRST: self.direct, FAR: self.passed, SECOND: self.near}[s]
        k = {FIRST: 0, FAR: 1, SECOND: 2}[s] * 2 + piece
        return pltpu.make_async_remote_copy(
            src_ref=self.g.at[self.STAGE[s][0] + piece, :, self.cols(n)], dst_ref=buffer.at[piece, :, self.cols(n)],
            send_sem=self.send.at[k], recv_sem=self.recv.at[k * self.steps + (0 if n is None else n)],
            device_id={"tp": to}, device_id_type=MESH)

    def run(self, s, term, out=None, out_sem=None):
        half = self.g.shape[1]
        lag = self.held.shape[0] - 1
        mine, other = self.STAGE[s]

        def leave(n):
            if s == OWN:
                return [pltpu.make_async_copy(self.g.at[mine + piece, :, self.cols(n)], out.at[piece, :, self.cols(n)],
                                              out_sem.at[n * 2 + piece]) for piece in range(2)]
            return [self.hop(s, piece, n) for piece in range(2)]

        def came(sets, n):
            for k in sets:
                for piece in range(2):
                    self.hop(k, piece, n).wait_recv()

        def body(n, _):
            @pl.when(n < self.steps)
            def _():
                t = term(n)
                self.held[lax.rem(n, lag + 1)] = t[: 2 * half]
                for piece in range(2):
                    self.g[other + piece, :, self.cols(n)] = t[(2 + piece) * half : (3 + piece) * half].astype(self.g.dtype)

            @pl.when((n > 0) & (n <= self.steps))
            def _():
                self.swap(s, n - 1).start()

            @pl.when(n >= lag)
            def _():
                m = n - lag
                self.swap(s, m).wait_recv()
                came({SECOND: (FAR,), OWN: (FIRST, SECOND)}.get(s, ()), m)
                more = {SECOND: (self.passed,), OWN: (self.direct, self.near)}.get(s, ())
                for piece in range(2):
                    total = self.held[lax.rem(m, lag + 1), piece * half : (piece + 1) * half]
                    for ref in (self.swapped.at[s], *more):
                        total += ref[piece, :, self.cols(m)].astype(jnp.float32)
                    if s == OWN:
                        total += self.g[mine + piece, :, self.cols(m)].astype(jnp.float32)
                    self.g[mine + piece, :, self.cols(m)] = total.astype(self.g.dtype)

            @pl.when(n > lag)
            def _():
                for c in leave(n - lag - 1):
                    c.start()

        lax.fori_loop(0, self.steps + lag, body, None)
        for c in leave(self.steps - 1):
            c.start()
        if s == OWN:
            def end(n, _):
                for c in leave(n):
                    c.wait()

            lax.fori_loop(0, self.steps, end, None)

    def sent(self):
        for s in range(4):
            self.swap(s, None).wait_send()
        for s in (FIRST, FAR, SECOND):
            for piece in range(2):
                self.hop(s, piece, None).wait_send()


def _norm(g, gain_ref):
    step = 16
    per = g.shape[1] // step
    gain = gain_ref[...].reshape(1, -1).astype(jnp.float32)

    def body(i, _):
        at = pl.ds(pl.multiple_of(lax.rem(i, per) * step, step), step)
        t = g[lax.div(i, per), at, :].astype(jnp.float32)
        scale = lax.rsqrt(jnp.mean(t * t, -1, keepdims=True) + 1e-6)
        g[lax.div(i, per), at, :] = (t * scale * gain).astype(g.dtype)

    lax.fori_loop(0, 2 * per, body, None)


def _mlp(n, h_ref, gain_ref, gate_ref, up_ref, down_ref, y_ref, g, swapped, direct, passed, near, held, hid, wgu, wd,
         g_send, g_recv, swap_send, swap_recv, hop_send, hop_recv, w_sem, io_sem, out_sem):
    around = _around(n)
    gather = Gather(g, g_send, g_recv, around)
    scatter = Scatter(g, swapped, direct, passed, near, held, (swap_send, swap_recv, hop_send, hop_recv), around)
    rows = 2 * g.shape[1]
    depth = g.shape[2]
    units = gate_ref.shape[1]
    tiles, steps = units // HIDE, scatter.steps
    early = 5 * tiles // 7

    def fetch(i, slot):
        at = pl.ds(pl.multiple_of(i * HIDE, HIDE), HIDE)
        return [pltpu.make_async_copy(ref.at[:, at], wgu.at[slot, k], w_sem.at[slot * 2 + k]) for k, ref in enumerate((gate_ref, up_ref))]

    def fetch_down(i, slot):
        return pltpu.make_async_copy(down_ref.at[:, scatter.cols(i)], wd.at[slot], w_sem.at[4 + slot])

    def hidden(s, place, first, end, then):
        def body(i, _):
            slot = lax.rem(i, 2)

            @pl.when(i + 1 < end)
            def _():
                for c in fetch(i + 1, 1 - slot):
                    c.start()

            for c in fetch(i, slot):
                c.wait()
            at = pl.ds(pl.multiple_of(i * HIDE, HIDE), HIDE)
            for part in range(2):
                t = g[4 * s + 2 * part : 4 * s + 2 * part + 2].reshape(rows, depth)
                gate = jnp.dot(t, wgu[slot, 0], preferred_element_type=jnp.float32)
                up = jnp.dot(t, wgu[slot, 1], preferred_element_type=jnp.float32)
                hid[place, part * rows : (part + 1) * rows, at] = (gate / (1 + jnp.exp(-gate)) * up).astype(hid.dtype)

        lax.fori_loop(first, end, body, None)
        if then is not None:
            for c in fetch(then, then % 2):
                c.start()

    def down(s, place, *out):
        def term(i):
            slot = lax.rem(i, 2)

            @pl.when(i + 1 < steps)
            def _():
                fetch_down(i + 1, 1 - slot).start()

            fetch_down(i, slot).wait()
            return jnp.dot(hid[place], wd[slot], preferred_element_type=jnp.float32)

        scatter.run(s, term, *out)
        if s != OWN:
            fetch_down(0, 0).start()

    load = pltpu.make_async_copy(h_ref, g.at[pl.ds(0, 2)], io_sem.at[0])
    load.start()
    for c in fetch(0, 0):
        c.start()
    fetch_down(0, 0).start()
    _enter(*around)
    load.wait()
    _norm(g, gain_ref)
    gather.start(4, 5, 2, 3, 9, 8)
    gather.arrived(2, 3)
    hidden(OWN, 1, 0, tiles, 0)
    gather.arrived(4, 5)
    gather.start(12, 13, sub=0)
    gather.start(12, 13, sub=1)
    gather.start(6, 7)
    gather.arrived(6, 7)
    hidden(FIRST, 0, 0, tiles, 0)
    gather.arrived(8, 9)
    gather.start(10, 11)
    gather.sent(4, 5, 2, 3, 9, 8)
    down(FIRST, 0)
    gather.arrived(10, 11)
    hidden(SECOND, 2, 0, early, 0)
    for sub in range(2):
        gather.arrived(12, 13, sub=sub)
        gather.start(14, 15, sub=sub)
    for sub in range(2):
        gather.arrived(14, 15, sub=sub)
    hidden(FAR, 0, 0, tiles, early)
    for sub in range(2):
        gather.sent(12, 13, 14, 15, sub=sub)
    gather.sent(6, 7, 10, 11)
    load = pltpu.make_async_copy(h_ref, g.at[pl.ds(12, 2)], io_sem.at[0])
    load.start()
    down(FAR, 0)
    hidden(SECOND, 2, early, tiles, None)
    down(SECOND, 2)
    load.wait()
    down(OWN, 1, y_ref, out_sem)
    scatter.sent()


def _buffers(half, depth, lag):
    piece = lambda k: pltpu.VMEM((k, half, depth), jnp.bfloat16)
    steps = depth // COLS
    buffers = [piece(16), pltpu.VMEM((4, 2, half, depth), jnp.bfloat16), piece(2), piece(2), piece(2), pltpu.VMEM((lag + 1, 2 * half, COLS), jnp.float32)]
    sems = [pltpu.SemaphoreType.DMA((k,)) for k in (20, 20, 4, 4 * steps, 6, 6 * steps)]
    return buffers, sems


def mlp(n, h, gain, gate, up, down):
    rows, depth = h.shape
    half = rows // 2
    units = gate.shape[1]
    buffers, sems = _buffers(half, depth, 2)
    any_space = pl.BlockSpec(memory_space=pl.ANY)
    y = pl.pallas_call(
        functools.partial(_mlp, n),
        out_shape=jax.ShapeDtypeStruct((2, half, depth), h.dtype),
        in_specs=[any_space, pl.BlockSpec(memory_space=pltpu.VMEM), any_space, any_space, any_space],
        out_specs=any_space,
        scratch_shapes=[*buffers, pltpu.VMEM((3, 2 * rows, units), h.dtype), pltpu.VMEM((2, 2, depth, HIDE), h.dtype),
                        pltpu.VMEM((2, units, COLS), h.dtype), *sems, pltpu.SemaphoreType.DMA((6,)), pltpu.SemaphoreType.DMA((1,)),
                        pltpu.SemaphoreType.DMA((2 * depth // COLS,))],
        compiler_params=pltpu.CompilerParams(collective_id=1, has_side_effects=True, vmem_limit_bytes=FULL),
        cost_estimate=pl.CostEstimate(flops=6 * rows * n * depth * units, transcendentals=rows * n * units,
                                      bytes_accessed=12 * depth * units),
    )(h.reshape(2, half, depth), gain, gate, up, down)
    return y.reshape(rows, depth)


def _turned(t, cos, sin):
    half = HEAD // 2
    t = t.astype(jnp.bfloat16).astype(jnp.float32)
    a, b = t[:, :half], t[:, half:]
    return jnp.concatenate([a * cos - b * sin, b * cos + a * sin], -1).astype(jnp.bfloat16)


def _attention(n, x_ref, gain_ref, wq_ref, wk_ref, wv_ref, wo_ref, y_ref, g, swapped, direct, passed, near, held, w, wo, queries, kv,
               top_s, mix_s, cos_s, sin_s, cos0_s, sin0_s, g_send, g_recv, swap_send, swap_recv, hop_send, hop_recv, w_sem, io_sem, out_sem):
    around = _around(n)
    gather = Gather(g, g_send, g_recv, around)
    scatter = Scatter(g, swapped, direct, passed, near, held, (swap_send, swap_recv, hop_send, hop_recv), around)
    half, depth = g.shape[1], g.shape[2]
    rows = 2 * half
    heads = wq_ref.shape[1] // HEAD
    cols = 2 * heads * half
    me = lax.axis_index("tp")
    core = lax.rem(me, 2)
    e = HEAD**-0.5 * LOG2E

    def chip(shift):
        return lax.rem(me - core + 2 * shift + n, n)

    def number(s, pair):
        shift = jnp.where(s == FIRST, 2 * pair - 1, jnp.where(s == SECOND, 1 - 2 * pair, jnp.where(s == FAR, 2, 0)))
        return 2 * chip(shift) + pair

    copies = [pltpu.make_async_copy(ref, w.at[:, pl.ds(at, ref.shape[1])], w_sem.at[k])
              for k, (ref, at) in enumerate(((wq_ref, 0), (wk_ref, heads * HEAD), (wv_ref, (heads + 1) * HEAD)))]
    copies.append(pltpu.make_async_copy(wo_ref, wo, w_sem.at[3]))

    def project(s, part, columns, sub=None):
        size = half if sub is None else half // 2
        start = (sub or 0) * size
        t = g[pl.ds(4 * s + 2 * part, 2), start : start + size, :].reshape(2 * size, depth)
        for c in columns:
            r = jnp.dot(t, w[:, c * HEAD : (c + 1) * HEAD], preferred_element_type=jnp.float32)
            for pair in range(2):
                piece = number(s, pair) + 2 * (core + part - 2 * core * part)
                z = r[pair * size : (pair + 1) * size]
                at = pl.ds(pl.multiple_of(piece * half + start, 32), size)
                if c == heads + 1:
                    kv[at, HEAD:] = z.astype(jnp.bfloat16)
                    continue
                c0, s0 = cos0_s[pl.ds(piece, 1), :], sin0_s[pl.ds(piece, 1), :]
                cos, sin = cos_s[start : start + size, :], sin_s[start : start + size, :]
                z = _turned(z, cos * c0 - sin * s0, sin * c0 + cos * s0)
                if c == heads:
                    kv[at, :HEAD] = z
                else:
                    queries[2 * s + pair, pl.ds(pl.multiple_of((part * heads + c) * half + start, 32), size), :] = z

    def begin(pair):
        top_s[pair] = jnp.full((1, cols), NEG, jnp.float32)
        mix_s[pair] = jnp.zeros((HEAD + 8, cols), jnp.float32)

    def attend(s, pair, first, end):
        lowest = number(s, pair) * half
        column = lax.broadcasted_iota(jnp.int32, (1, cols), 1)
        behind = jnp.where(column < heads * half, core * rows, (1 - core) * rows)
        place = lax.rem(column, half) + behind + lowest
        ones = jnp.ones((8, BK), jnp.bfloat16)

        def block(j, masked):
            here = pl.ds(pl.multiple_of(j * BK, BK), BK)
            keys = kv[here, :HEAD]
            values = jnp.concatenate([kv[here, HEAD:].T, ones], axis=0)
            strips = range(0, cols, WIDE)
            scores = [_dot(keys, queries[2 * s + pair, at : at + WIDE, :], 1, 1) for at in strips]
            weights, keeps = [], []
            for at, z in zip(strips, scores):
                if masked:
                    key = lax.broadcasted_iota(jnp.int32, z.shape, 0) + j * BK
                    z = jnp.where(key <= place[:, at : at + WIDE], z, HIDDEN)
                old = top_s[pair, :, at : at + WIDE]
                top = jnp.maximum(old, z.max(axis=0, keepdims=True))
                top_s[pair, :, at : at + WIDE] = top
                weights.append(jnp.exp2((z - top) * e).astype(jnp.bfloat16))
                keeps.append(jnp.exp2((old - top) * e))
            for at, p, keep in zip(strips, weights, keeps):
                mix_s[pair, :, at : at + WIDE] = mix_s[pair, :, at : at + WIDE] * keep + _dot(values, p, 1, 0)

        whole = lax.div(lowest + 1, BK)
        last = lax.div(lowest + rows + half + BK - 1, BK)
        whole = jnp.minimum(jnp.maximum(whole, first), end)
        last = jnp.minimum(jnp.maximum(last, first), end)
        lax.fori_loop(first, whole, lambda j, _: block(j, False), None)
        lax.fori_loop(whole, last, lambda j, _: block(j, True), None)

    def done(s, pair):
        queries[2 * s + pair] = (mix_s[pair, :HEAD, :] * (1 / mix_s[pair, HEAD : HEAD + 1, :])).T.astype(jnp.bfloat16)

    def pairs(body):
        lax.fori_loop(0, 2, lambda pair, _: body(pair), None)

    def attended(s):
        def body(pair):
            begin(pair)
            attend(s, pair, 0, kv.shape[0] // BK)
            done(s, pair)

        pairs(body)

    def some(s, shift):
        per = 2 * rows // BK
        first = lax.div(chip(shift), 2) * per
        pairs(lambda pair: attend(s, pair, first, first + per))

    def spread(s, *out):
        def term(i):
            t = [jnp.concatenate([queries[2 * s + pair, (part * heads + h) * half : (part * heads + h + 1) * half, :] for h in range(heads)], 1)
                 for part in range(2) for pair in range(2)]
            return jnp.dot(jnp.concatenate(t, 0), wo[:, scatter.cols(i)], preferred_element_type=jnp.float32)

        scatter.run(s, term, *out)

    load = pltpu.make_async_copy(x_ref, g.at[pl.ds(0, 2)], io_sem.at[0])
    load.start()
    _enter(*around)
    load.wait()
    _norm(g, gain_ref)
    gather.start(4, 5, 2, 3, 9, 8)
    for c in copies:
        c.start()
    turn = lax.broadcasted_iota(jnp.int32, (1, HEAD // 2), 1).astype(jnp.float32) / (HEAD // 2)
    frequency = jnp.exp2(-turn * math.log2(THETA))
    angle = lax.broadcasted_iota(jnp.int32, cos_s.shape, 0).astype(jnp.float32) * frequency
    cos_s[...], sin_s[...] = jnp.cos(angle), jnp.sin(angle)
    angle = (lax.broadcasted_iota(jnp.int32, cos0_s.shape, 0) * half).astype(jnp.float32) * frequency
    cos0_s[...], sin0_s[...] = jnp.cos(angle), jnp.sin(angle)
    for c in copies:
        c.wait()
    every, q_columns, kv_columns = range(heads + 2), range(heads), range(heads, heads + 2)

    def early(i, _):
        @pl.when(i == 1)
        def _():
            gather.arrived(2, 3)

        @pl.when(i == 2)
        def _():
            gather.arrived(4, 5)
            gather.start(12, 13, sub=0)
            gather.start(12, 13, sub=1)
            gather.start(6, 7)

        @pl.when(i == 3)
        def _():
            gather.arrived(6, 7)

        @pl.when(i == 4)
        def _():
            gather.arrived(8, 9)
            gather.start(10, 11)

        @pl.when(i == 5)
        def _():
            gather.arrived(10, 11)

        project(lax.div(i, 2), lax.rem(i, 2), every)

    lax.fori_loop(0, 6, early, None)
    pairs(begin)
    lax.fori_loop(0, 3, lambda i, _: some(FIRST, i - 1), None)
    gather.sent(4, 5, 2, 3, 9, 8)
    for sub in range(2):
        gather.arrived(12, 13, sub=sub)
        gather.start(14, 15, sub=sub)
        project(FAR, 0, kv_columns, sub)
        gather.arrived(14, 15, sub=sub)
        project(FAR, 1, kv_columns, sub)
    some(FIRST, 2)
    pairs(lambda pair: done(FIRST, pair))
    spread(FIRST)
    lax.fori_loop(0, 2, lambda part, _: project(FAR, part, q_columns), None)
    for sub in range(2):
        gather.sent(12, 13, 14, 15, sub=sub)
    gather.sent(6, 7, 10, 11)
    load = pltpu.make_async_copy(x_ref, g.at[pl.ds(12, 2)], io_sem.at[0])
    load.start()
    attended(FAR)
    spread(FAR)
    attended(SECOND)
    spread(SECOND)
    attended(OWN)
    load.wait()
    spread(OWN, y_ref, out_sem)
    scatter.sent()


def attention(n, x, gain, wq, wk, wv, wo):
    rows, depth = x.shape
    half = rows // 2
    heads = wq.shape[1] // HEAD
    cols = 2 * heads * half
    buffers, sems = _buffers(half, depth, 2)
    any_space, vmem = pl.BlockSpec(memory_space=pl.ANY), pl.BlockSpec(memory_space=pltpu.VMEM)
    trig = [pltpu.VMEM((k, HEAD // 2), jnp.float32) for k in (half, half, 2 * n, 2 * n)]
    y = pl.pallas_call(
        functools.partial(_attention, n),
        out_shape=jax.ShapeDtypeStruct((2, half, depth), x.dtype),
        in_specs=[any_space, vmem, any_space, any_space, any_space, any_space],
        out_specs=any_space,
        scratch_shapes=[*buffers, pltpu.VMEM((depth, (heads + 2) * HEAD), x.dtype), pltpu.VMEM((heads * HEAD, depth), x.dtype),
                        pltpu.VMEM((8, cols, HEAD), x.dtype), pltpu.VMEM((n * rows, 2 * HEAD), x.dtype),
                        pltpu.VMEM((2, 1, cols), jnp.float32),
                        pltpu.VMEM((2, HEAD + 8, cols), jnp.float32), *trig, *sems, pltpu.SemaphoreType.DMA((4,)),
                        pltpu.SemaphoreType.DMA((1,)), pltpu.SemaphoreType.DMA((2 * depth // COLS,))],
        compiler_params=pltpu.CompilerParams(collective_id=0, has_side_effects=True, vmem_limit_bytes=FULL),
        cost_estimate=pl.CostEstimate(flops=2 * rows * n * depth * (2 * heads + 2) * HEAD, transcendentals=rows * n * rows * n,
                                      bytes_accessed=4 * depth * (2 * heads + 2) * HEAD),
    )(x.reshape(2, half, depth), gain, wq, wk, wv, wo)
    return y.reshape(rows, depth)


def solution(mesh):
    n = mesh.shape["tp"]

    def step(x, gain_a, wq, wk, wv, wo, gain_m, w_gate, w_up, w_down):
        h = attention(n, x, gain_a, wq, wk, wv, wo)
        return mlp(n, h, gain_m, w_gate, w_up, w_down)

    tokens, columns, rows_of = P(("dp", "tp"), None), P(None, "tp"), P("tp", None)
    return jax.shard_map(
        step,
        mesh=mesh,
        in_specs=(tokens, P(None), columns, columns, columns, rows_of, P(None), columns, columns, rows_of),
        out_specs=tokens,
        check_vma=False,
    )
```

```python
import functools
import math

import jax
import jax.numpy as jnp
from jax import lax
from jax.experimental import pallas as pl
from jax.experimental.pallas import tpu as pltpu
from jax.sharding import PartitionSpec as P

NEG = -1e30
HIDDEN = 2 * NEG
LOG2E = 1.4426950408889634
HEAD = 256
THETA = 10000
BK = 256
WIDE = 256


def _dot(a, b, ca, cb):
    return lax.dot_general(a, b, (((ca,), (cb,)), ((), ())), preferred_element_type=jnp.float32)


MESH = pl.DeviceIdType.MESH
FULL = 67_043_328
COLS = 512
HIDE = 256
OWN, FIRST, SECOND, FAR = range(4)


def _around(n):
    me = lax.axis_index("tp")
    return lax.rem(me + 2, n), lax.rem(me + n - 2, n), me + 1 - 2 * lax.rem(me, 2)


def _enter(*others):
    barrier = pltpu.get_barrier_semaphore()
    for other in others:
        pl.semaphore_signal(barrier, inc=1, device_id={"tp": other}, device_id_type=MESH)
    pl.semaphore_wait(barrier, len(others))


class Gather:
    def __init__(self, g, send, recv, around):
        self.g, self.sems, self.around = g, (send, recv), around

    PATH = {4: (0, "right"), 5: (1, "left"), 9: (1, "right"), 8: (0, "left"), 12: (4, "right"), 13: (5, "left"),
            2: (0, "twin"), 3: (1, "twin"), 6: (4, "twin"), 7: (5, "twin"), 10: (8, "twin"), 11: (9, "twin"), 14: (12, "twin"), 15: (13, "twin")}

    def copies(self, slots, sub):
        right, left, twin = self.around
        rows = self.g.shape[1]
        at = pl.ds(0, rows) if sub is None else pl.ds(sub * (rows // 2), rows // 2)
        made = []
        for slot in slots:
            source, to = self.PATH[slot]
            sem = slot + (4 if sub == 1 else 0)
            made.append(pltpu.make_async_remote_copy(
                src_ref=self.g.at[source, at], dst_ref=self.g.at[slot, at], send_sem=self.sems[0].at[sem], recv_sem=self.sems[1].at[sem],
                device_id={"tp": {"right": right, "left": left, "twin": twin}[to]}, device_id_type=MESH))
        return made

    def start(self, *slots, sub=None):
        for c in self.copies(slots, sub):
            c.start()

    def arrived(self, *slots, sub=None):
        for c in self.copies(slots, sub):
            c.wait_recv()

    def sent(self, *slots, sub=None):
        for c in self.copies(slots, sub):
            c.wait_send()


class Scatter:
    STAGE = {FIRST: (0, 2), FAR: (4, 6), SECOND: (8, 10), OWN: (12, 14)}

    def __init__(self, g, swapped, direct, passed, near, held, sems, around):
        self.g, self.swapped, self.direct, self.passed, self.near, self.held, self.around = g, swapped, direct, passed, near, held, around
        self.swap_send, self.swap_recv, self.send, self.recv = sems
        self.steps = g.shape[2] // COLS

    def cols(self, n):
        return pl.ds(0, self.g.shape[2]) if n is None else pl.ds(pl.multiple_of(n * COLS, COLS), COLS)

    def swap(self, s, n):
        return pltpu.make_async_remote_copy(
            src_ref=self.g.at[pl.ds(self.STAGE[s][1], 2), :, self.cols(n)], dst_ref=self.swapped.at[s, :, :, self.cols(n)],
            send_sem=self.swap_send.at[s], recv_sem=self.swap_recv.at[s * self.steps + (0 if n is None else n)],
            device_id={"tp": self.around[2]}, device_id_type=MESH)

    def hop(self, s, piece, n):
        right, left, _ = self.around
        to = left if (s == FIRST) == (piece == 0) else right
        buffer = {FIRST: self.direct, FAR: self.passed, SECOND: self.near}[s]
        k = {FIRST: 0, FAR: 1, SECOND: 2}[s] * 2 + piece
        return pltpu.make_async_remote_copy(
            src_ref=self.g.at[self.STAGE[s][0] + piece, :, self.cols(n)], dst_ref=buffer.at[piece, :, self.cols(n)],
            send_sem=self.send.at[k], recv_sem=self.recv.at[k * self.steps + (0 if n is None else n)],
            device_id={"tp": to}, device_id_type=MESH)

    def run(self, s, term, out=None, out_sem=None):
        half = self.g.shape[1]
        lag = self.held.shape[0] - 1
        mine, other = self.STAGE[s]

        def leave(n):
            if s == OWN:
                return [pltpu.make_async_copy(self.g.at[mine + piece, :, self.cols(n)], out.at[piece, :, self.cols(n)],
                                              out_sem.at[n * 2 + piece]) for piece in range(2)]
            return [self.hop(s, piece, n) for piece in range(2)]

        def came(sets, n):
            for k in sets:
                for piece in range(2):
                    self.hop(k, piece, n).wait_recv()

        def body(n, _):
            @pl.when(n < self.steps)
            def _():
                t = term(n)
                self.held[lax.rem(n, lag + 1)] = t[: 2 * half]
                for piece in range(2):
                    self.g[other + piece, :, self.cols(n)] = t[(2 + piece) * half : (3 + piece) * half].astype(self.g.dtype)

            @pl.when((n > 0) & (n <= self.steps))
            def _():
                self.swap(s, n - 1).start()

            @pl.when(n >= lag)
            def _():
                m = n - lag
                self.swap(s, m).wait_recv()
                came({SECOND: (FAR,), OWN: (FIRST, SECOND)}.get(s, ()), m)
                more = {SECOND: (self.passed,), OWN: (self.direct, self.near)}.get(s, ())
                for piece in range(2):
                    total = self.held[lax.rem(m, lag + 1), piece * half : (piece + 1) * half]
                    for ref in (self.swapped.at[s], *more):
                        total += ref[piece, :, self.cols(m)].astype(jnp.float32)
                    if s == OWN:
                        total += self.g[mine + piece, :, self.cols(m)].astype(jnp.float32)
                    self.g[mine + piece, :, self.cols(m)] = total.astype(self.g.dtype)

            @pl.when(n > lag)
            def _():
                for c in leave(n - lag - 1):
                    c.start()

        lax.fori_loop(0, self.steps + lag, body, None)
        for c in leave(self.steps - 1):
            c.start()
        if s == OWN:
            def end(n, _):
                for c in leave(n):
                    c.wait()

            lax.fori_loop(0, self.steps, end, None)

    def sent(self):
        for s in range(4):
            self.swap(s, None).wait_send()
        for s in (FIRST, FAR, SECOND):
            for piece in range(2):
                self.hop(s, piece, None).wait_send()


def _norm(g, gain_ref):
    step = 16
    several = 4 if g.shape[1] % (4 * step) == 0 else 1
    per = g.shape[1] // (several * step)
    gain = gain_ref[...].reshape(1, -1).astype(jnp.float32)

    def body(i, _):
        slot = lax.div(i, per)
        at = [pl.ds(pl.multiple_of((lax.rem(i, per) * several + k) * step, step), step) for k in range(several)]
        scales = []
        for rows in at:
            t = g[slot, rows, :].astype(jnp.float32)
            scales.append(lax.rsqrt(jnp.mean(t * t, -1, keepdims=True) + 1e-6))
        for rows, scale in zip(at, scales):
            g[slot, rows, :] = (g[slot, rows, :].astype(jnp.float32) * scale * gain).astype(g.dtype)

    lax.fori_loop(0, 2 * per, body, None)


def _mlp(n, h_ref, gain_ref, gate_ref, up_ref, down_ref, y_ref, g, swapped, direct, passed, near, held, hid, wgu, wd,
         g_send, g_recv, swap_send, swap_recv, hop_send, hop_recv, w_sem, io_sem, out_sem):
    around = _around(n)
    gather = Gather(g, g_send, g_recv, around)
    scatter = Scatter(g, swapped, direct, passed, near, held, (swap_send, swap_recv, hop_send, hop_recv), around)
    rows = 2 * g.shape[1]
    depth = g.shape[2]
    units = gate_ref.shape[1]
    tiles, steps = units // HIDE, scatter.steps
    early = 5 * tiles // 7

    def fetch(i, slot):
        at = pl.ds(pl.multiple_of(i * HIDE, HIDE), HIDE)
        return [pltpu.make_async_copy(ref.at[:, at], wgu.at[slot, k], w_sem.at[slot * 2 + k]) for k, ref in enumerate((gate_ref, up_ref))]

    def fetch_down(i, slot):
        return pltpu.make_async_copy(down_ref.at[:, scatter.cols(i)], wd.at[slot], w_sem.at[4 + slot])

    def hidden(s, place, first, end, then):
        def body(i, _):
            slot = lax.rem(i, 2)

            @pl.when(i + 1 < end)
            def _():
                for c in fetch(i + 1, 1 - slot):
                    c.start()

            for c in fetch(i, slot):
                c.wait()
            at = pl.ds(pl.multiple_of(i * HIDE, HIDE), HIDE)
            for part in range(2):
                t = g[4 * s + 2 * part : 4 * s + 2 * part + 2].reshape(rows, depth)
                gate = jnp.dot(t, wgu[slot, 0], preferred_element_type=jnp.float32)
                up = jnp.dot(t, wgu[slot, 1], preferred_element_type=jnp.float32)
                hid[place, part * rows : (part + 1) * rows, at] = (gate / (1 + jnp.exp(-gate)) * up).astype(hid.dtype)

        lax.fori_loop(first, end, body, None)
        if then is not None:
            for c in fetch(then, then % 2):
                c.start()

    def down(s, place, *out):
        def term(i):
            slot = lax.rem(i, 2)

            @pl.when(i + 1 < steps)
            def _():
                fetch_down(i + 1, 1 - slot).start()

            fetch_down(i, slot).wait()
            return jnp.dot(hid[place], wd[slot], preferred_element_type=jnp.float32)

        scatter.run(s, term, *out)
        if s != OWN:
            fetch_down(0, 0).start()

    load = pltpu.make_async_copy(h_ref, g.at[pl.ds(0, 2)], io_sem.at[0])
    load.start()
    for c in fetch(0, 0):
        c.start()
    fetch_down(0, 0).start()
    _enter(*around)
    load.wait()
    _norm(g, gain_ref)
    gather.start(4, 5, 2, 3, 9, 8)
    gather.arrived(2, 3)
    hidden(OWN, 1, 0, tiles, 0)
    gather.arrived(4, 5)
    gather.start(12, 13, sub=0)
    gather.start(12, 13, sub=1)
    gather.start(6, 7)
    gather.arrived(6, 7)
    hidden(FIRST, 0, 0, tiles, 0)
    gather.arrived(8, 9)
    gather.start(10, 11)
    gather.sent(4, 5, 2, 3, 9, 8)
    down(FIRST, 0)
    gather.arrived(10, 11)
    hidden(SECOND, 2, 0, early, 0)
    for sub in range(2):
        gather.arrived(12, 13, sub=sub)
        gather.start(14, 15, sub=sub)
    for sub in range(2):
        gather.arrived(14, 15, sub=sub)
    hidden(FAR, 0, 0, tiles, early)
    for sub in range(2):
        gather.sent(12, 13, 14, 15, sub=sub)
    gather.sent(6, 7, 10, 11)
    load = pltpu.make_async_copy(h_ref, g.at[pl.ds(12, 2)], io_sem.at[0])
    load.start()
    down(FAR, 0)
    hidden(SECOND, 2, early, tiles, None)
    down(SECOND, 2)
    load.wait()
    down(OWN, 1, y_ref, out_sem)
    scatter.sent()


def _buffers(half, depth, lag):
    piece = lambda k: pltpu.VMEM((k, half, depth), jnp.bfloat16)
    steps = depth // COLS
    buffers = [piece(16), pltpu.VMEM((4, 2, half, depth), jnp.bfloat16), piece(2), piece(2), piece(2), pltpu.VMEM((lag + 1, 2 * half, COLS), jnp.float32)]
    sems = [pltpu.SemaphoreType.DMA((k,)) for k in (20, 20, 4, 4 * steps, 6, 6 * steps)]
    return buffers, sems


def mlp(n, h, gain, gate, up, down):
    rows, depth = h.shape
    half = rows // 2
    units = gate.shape[1]
    buffers, sems = _buffers(half, depth, 2)
    any_space = pl.BlockSpec(memory_space=pl.ANY)
    y = pl.pallas_call(
        functools.partial(_mlp, n),
        out_shape=jax.ShapeDtypeStruct((2, half, depth), h.dtype),
        in_specs=[any_space, pl.BlockSpec(memory_space=pltpu.VMEM), any_space, any_space, any_space],
        out_specs=any_space,
        scratch_shapes=[*buffers, pltpu.VMEM((3, 2 * rows, units), h.dtype), pltpu.VMEM((2, 2, depth, HIDE), h.dtype),
                        pltpu.VMEM((2, units, COLS), h.dtype), *sems, pltpu.SemaphoreType.DMA((6,)), pltpu.SemaphoreType.DMA((1,)),
                        pltpu.SemaphoreType.DMA((2 * depth // COLS,))],
        compiler_params=pltpu.CompilerParams(collective_id=1, has_side_effects=True, vmem_limit_bytes=FULL),
        cost_estimate=pl.CostEstimate(flops=6 * rows * n * depth * units, transcendentals=rows * n * units,
                                      bytes_accessed=12 * depth * units),
    )(h.reshape(2, half, depth), gain, gate, up, down)
    return y.reshape(rows, depth)


def _turned(t, cos, sin):
    half = HEAD // 2
    t = t.astype(jnp.bfloat16).astype(jnp.float32)
    a, b = t[:, :half], t[:, half:]
    return jnp.concatenate([a * cos - b * sin, b * cos + a * sin], -1).astype(jnp.bfloat16)


def _attention(n, x_ref, gain_ref, wq_ref, wk_ref, wv_ref, wo_ref, y_ref, g, swapped, direct, passed, near, held, w, wo, queries, kv,
               top_s, mix_s, cos_s, sin_s, cos0_s, sin0_s, g_send, g_recv, swap_send, swap_recv, hop_send, hop_recv, w_sem, io_sem, out_sem):
    around = _around(n)
    gather = Gather(g, g_send, g_recv, around)
    scatter = Scatter(g, swapped, direct, passed, near, held, (swap_send, swap_recv, hop_send, hop_recv), around)
    half, depth = g.shape[1], g.shape[2]
    rows = 2 * half
    heads = wq_ref.shape[1] // HEAD
    cols = 2 * heads * half
    me = lax.axis_index("tp")
    core = lax.rem(me, 2)
    e = HEAD**-0.5 * LOG2E

    def chip(shift):
        return lax.rem(me - core + 2 * shift + n, n)

    def number(s, pair):
        shift = jnp.where(s == FIRST, 2 * pair - 1, jnp.where(s == SECOND, 1 - 2 * pair, jnp.where(s == FAR, 2, 0)))
        return 2 * chip(shift) + pair

    copies = [pltpu.make_async_copy(ref, w.at[:, pl.ds(at, ref.shape[1])], w_sem.at[k])
              for k, (ref, at) in enumerate(((wq_ref, 0), (wk_ref, heads * HEAD), (wv_ref, (heads + 1) * HEAD)))]
    copies.append(pltpu.make_async_copy(wo_ref, wo, w_sem.at[3]))

    def project(s, part, columns, sub=None):
        size = half if sub is None else half // 2
        start = (sub or 0) * size
        t = g[pl.ds(4 * s + 2 * part, 2), start : start + size, :].reshape(2 * size, depth)
        for c in columns:
            r = jnp.dot(t, w[:, c * HEAD : (c + 1) * HEAD], preferred_element_type=jnp.float32)
            for pair in range(2):
                piece = number(s, pair) + 2 * (core + part - 2 * core * part)
                z = r[pair * size : (pair + 1) * size]
                at = pl.ds(pl.multiple_of(piece * half + start, 32), size)
                if c == heads + 1:
                    kv[at, HEAD:] = z.astype(jnp.bfloat16)
                    continue
                c0, s0 = cos0_s[pl.ds(piece, 1), :], sin0_s[pl.ds(piece, 1), :]
                cos, sin = cos_s[start : start + size, :], sin_s[start : start + size, :]
                z = _turned(z, cos * c0 - sin * s0, sin * c0 + cos * s0)
                if c == heads:
                    kv[at, :HEAD] = z
                else:
                    queries[2 * s + pair, pl.ds(pl.multiple_of((part * heads + c) * half + start, 32), size), :] = z

    def begin(pair):
        top_s[pair] = jnp.full((1, cols), NEG, jnp.float32)
        mix_s[pair] = jnp.zeros((HEAD + 8, cols), jnp.float32)

    def attend(s, pair, first, end):
        lowest = number(s, pair) * half
        column = lax.broadcasted_iota(jnp.int32, (1, cols), 1)
        behind = jnp.where(column < heads * half, core * rows, (1 - core) * rows)
        place = lax.rem(column, half) + behind + lowest
        ones = jnp.ones((8, BK), jnp.bfloat16)

        def block(j, masked):
            here = pl.ds(pl.multiple_of(j * BK, BK), BK)
            keys = kv[here, :HEAD]
            values = jnp.concatenate([kv[here, HEAD:].T, ones], axis=0)
            strips = range(0, cols, WIDE)
            scores = [_dot(keys, queries[2 * s + pair, at : at + WIDE, :], 1, 1) for at in strips]
            weights, keeps = [], []
            for at, z in zip(strips, scores):
                if masked:
                    key = lax.broadcasted_iota(jnp.int32, z.shape, 0) + j * BK
                    z = jnp.where(key <= place[:, at : at + WIDE], z, HIDDEN)
                old = top_s[pair, :, at : at + WIDE]
                top = jnp.maximum(old, z.max(axis=0, keepdims=True))
                top_s[pair, :, at : at + WIDE] = top
                weights.append(jnp.exp2((z - top) * e).astype(jnp.bfloat16))
                keeps.append(jnp.exp2((old - top) * e))
            for at, p, keep in zip(strips, weights, keeps):
                mix_s[pair, :, at : at + WIDE] = mix_s[pair, :, at : at + WIDE] * keep + _dot(values, p, 1, 0)

        whole = lax.div(lowest + 1, BK)
        last = lax.div(lowest + rows + half + BK - 1, BK)
        whole = jnp.minimum(jnp.maximum(whole, first), end)
        last = jnp.minimum(jnp.maximum(last, first), end)
        lax.fori_loop(first, whole, lambda j, _: block(j, False), None)
        lax.fori_loop(whole, last, lambda j, _: block(j, True), None)

    def done(s, pair):
        queries[2 * s + pair] = (mix_s[pair, :HEAD, :] * (1 / mix_s[pair, HEAD : HEAD + 1, :])).T.astype(jnp.bfloat16)

    def pairs(body):
        lax.fori_loop(0, 2, lambda pair, _: body(pair), None)

    def attended(s):
        def body(pair):
            begin(pair)
            attend(s, pair, 0, kv.shape[0] // BK)
            done(s, pair)

        pairs(body)

    def some(s, shift):
        per = 2 * rows // BK
        first = lax.div(chip(shift), 2) * per
        pairs(lambda pair: attend(s, pair, first, first + per))

    def spread(s, *out):
        def term(i):
            t = [jnp.concatenate([queries[2 * s + pair, (part * heads + h) * half : (part * heads + h + 1) * half, :] for h in range(heads)], 1)
                 for part in range(2) for pair in range(2)]
            return jnp.dot(jnp.concatenate(t, 0), wo[:, scatter.cols(i)], preferred_element_type=jnp.float32)

        scatter.run(s, term, *out)

    load = pltpu.make_async_copy(x_ref, g.at[pl.ds(0, 2)], io_sem.at[0])
    load.start()
    _enter(*around)
    load.wait()
    _norm(g, gain_ref)
    gather.start(4, 5, 2, 3, 9, 8)
    for c in copies:
        c.start()
    turn = lax.broadcasted_iota(jnp.int32, (1, HEAD // 2), 1).astype(jnp.float32) / (HEAD // 2)
    frequency = jnp.exp2(-turn * math.log2(THETA))
    angle = lax.broadcasted_iota(jnp.int32, cos_s.shape, 0).astype(jnp.float32) * frequency
    cos_s[...], sin_s[...] = jnp.cos(angle), jnp.sin(angle)
    angle = (lax.broadcasted_iota(jnp.int32, cos0_s.shape, 0) * half).astype(jnp.float32) * frequency
    cos0_s[...], sin0_s[...] = jnp.cos(angle), jnp.sin(angle)
    for c in copies:
        c.wait()
    every, q_columns, kv_columns = range(heads + 2), range(heads), range(heads, heads + 2)

    def early(i, _):
        @pl.when(i == 1)
        def _():
            gather.arrived(2, 3)

        @pl.when(i == 2)
        def _():
            gather.arrived(4, 5)
            gather.start(12, 13, sub=0)
            gather.start(12, 13, sub=1)
            gather.start(6, 7)

        @pl.when(i == 3)
        def _():
            gather.arrived(6, 7)

        @pl.when(i == 4)
        def _():
            gather.arrived(8, 9)
            gather.start(10, 11)

        @pl.when(i == 5)
        def _():
            gather.arrived(10, 11)

        project(lax.div(i, 2), lax.rem(i, 2), every)

    lax.fori_loop(0, 6, early, None)
    pairs(begin)
    lax.fori_loop(0, 3, lambda i, _: some(FIRST, i - 1), None)
    gather.sent(4, 5, 2, 3, 9, 8)
    for sub in range(2):
        gather.arrived(12, 13, sub=sub)
        gather.start(14, 15, sub=sub)
        project(FAR, 0, kv_columns, sub)
        gather.arrived(14, 15, sub=sub)
        project(FAR, 1, kv_columns, sub)
    some(FIRST, 2)
    pairs(lambda pair: done(FIRST, pair))
    spread(FIRST)
    lax.fori_loop(0, 2, lambda part, _: project(FAR, part, q_columns), None)
    for sub in range(2):
        gather.sent(12, 13, 14, 15, sub=sub)
    gather.sent(6, 7, 10, 11)
    load = pltpu.make_async_copy(x_ref, g.at[pl.ds(12, 2)], io_sem.at[0])
    load.start()
    attended(FAR)
    spread(FAR)
    attended(SECOND)
    spread(SECOND)
    attended(OWN)
    load.wait()
    spread(OWN, y_ref, out_sem)
    scatter.sent()


def attention(n, x, gain, wq, wk, wv, wo):
    rows, depth = x.shape
    half = rows // 2
    heads = wq.shape[1] // HEAD
    cols = 2 * heads * half
    buffers, sems = _buffers(half, depth, 2)
    any_space, vmem = pl.BlockSpec(memory_space=pl.ANY), pl.BlockSpec(memory_space=pltpu.VMEM)
    trig = [pltpu.VMEM((k, HEAD // 2), jnp.float32) for k in (half, half, 2 * n, 2 * n)]
    y = pl.pallas_call(
        functools.partial(_attention, n),
        out_shape=jax.ShapeDtypeStruct((2, half, depth), x.dtype),
        in_specs=[any_space, vmem, any_space, any_space, any_space, any_space],
        out_specs=any_space,
        scratch_shapes=[*buffers, pltpu.VMEM((depth, (heads + 2) * HEAD), x.dtype), pltpu.VMEM((heads * HEAD, depth), x.dtype),
                        pltpu.VMEM((8, cols, HEAD), x.dtype), pltpu.VMEM((n * rows, 2 * HEAD), x.dtype),
                        pltpu.VMEM((2, 1, cols), jnp.float32),
                        pltpu.VMEM((2, HEAD + 8, cols), jnp.float32), *trig, *sems, pltpu.SemaphoreType.DMA((4,)),
                        pltpu.SemaphoreType.DMA((1,)), pltpu.SemaphoreType.DMA((2 * depth // COLS,))],
        compiler_params=pltpu.CompilerParams(collective_id=0, has_side_effects=True, vmem_limit_bytes=FULL),
        cost_estimate=pl.CostEstimate(flops=2 * rows * n * depth * (2 * heads + 2) * HEAD, transcendentals=rows * n * rows * n,
                                      bytes_accessed=4 * depth * (2 * heads + 2) * HEAD),
    )(x.reshape(2, half, depth), gain, wq, wk, wv, wo)
    return y.reshape(rows, depth)


def solution(mesh):
    n = mesh.shape["tp"]

    def step(x, gain_a, wq, wk, wv, wo, gain_m, w_gate, w_up, w_down):
        h = attention(n, x, gain_a, wq, wk, wv, wo)
        return mlp(n, h, gain_m, w_gate, w_up, w_down)

    tokens, columns, rows_of = P(("dp", "tp"), None), P(None, "tp"), P("tp", None)
    return jax.shard_map(
        step,
        mesh=mesh,
        in_specs=(tokens, P(None), columns, columns, columns, rows_of, P(None), columns, columns, rows_of),
        out_specs=tokens,
        check_vma=False,
    )
```
